8 devices in a mesh: dp: 1 (over z), tp: 8 (over y, x, core).
Axes of the slice: x: 2, y: 2, z: 1, core: 2. Of those that a mesh axis runs over, the one named last changes fastest.
Arguments:
- x_in: bfloat16 [1024, 6144], P(('dp', 'tp'))
- dy_in: bfloat16 [1024, 6144], P(('dp', 'tp'))
- w_q: bfloat16 [6144, 48, 128], P(None, 'tp')
- w_k: bfloat16 [6144, 1, 128], replicated
- w_v: bfloat16 [6144, 1, 128], replicated
- w_o: bfloat16 [48, 128, 6144], P('tp')
Outputs:
- output 1: bfloat16 [1024, 6144], P(('dp', 'tp'))
- output 2: float32 [6144, 48, 128], P('dp', 'tp')
- output 3: float32 [48, 128, 6144], P(('dp', 'tp'))
- output 4: float32 [6144, 128], P(('dp', 'tp'))
- output 5: float32 [6144, 128], P(('dp', 'tp'))
All inputs are finite; a program needn't handle non-finite values.
Results may differ from the reference program's by a relative error of at most 0.00989535.
Values are sent between devices in bfloat16 or wider.
A program may use at most 1 GiB of HBM per device.

```python
import jax
import jax.numpy as jnp
from jax import lax

D = 6144
HEADS = 48
KV_HEADS = 1
HEAD = 128
TOKENS = 1024
MODEL = 8

HEADS_DEV = HEADS // MODEL
REPL = MODEL // KV_HEADS
SCALE = HEAD ** -0.5


def setup_inputs(seed: int = 0, part: int = 0) -> dict:
    part_key = jax.random.fold_in(jax.random.key(seed), part)
    key_x, key_dy = jax.random.split(part_key)
    key_q, key_k, key_v, key_o = jax.random.split(jax.random.key(seed + 1), 4)
    fan_scale = D ** -0.5
    x_in = jax.random.normal(key_x, (TOKENS, D), jnp.float32).astype(jnp.bfloat16)
    dy_in = jax.random.normal(key_dy, (TOKENS, D), jnp.float32).astype(jnp.bfloat16)
    w_q = (jax.random.normal(key_q, (D, HEADS, HEAD), jnp.float32) * fan_scale).astype(jnp.bfloat16)
    w_k = (jax.random.normal(key_k, (D, KV_HEADS, HEAD), jnp.float32) * fan_scale).astype(jnp.bfloat16)
    w_v = (jax.random.normal(key_v, (D, KV_HEADS, HEAD), jnp.float32) * fan_scale).astype(jnp.bfloat16)
    w_o = (jax.random.normal(key_o, (HEADS, HEAD, D), jnp.float32) * fan_scale).astype(jnp.bfloat16)
    return dict(x_in=x_in, dy_in=dy_in, w_q=w_q, w_k=w_k, w_v=w_v, w_o=w_o)


def reference(x_in, dy_in, w_q, w_k, w_v, w_o):
    f32 = jnp.float32
    bf16 = jnp.bfloat16
    x_wide = x_in.astype(f32)
    dy_wide = dy_in.astype(f32)
    causal = lax.broadcasted_iota(jnp.int32, (TOKENS, TOKENS), 0) >= lax.broadcasted_iota(jnp.int32, (TOKENS, TOKENS), 1)
    wq_dev = jnp.transpose(w_q.reshape(D, MODEL, HEADS_DEV, HEAD), (1, 0, 2, 3))
    wo_dev = w_o.reshape(MODEL, HEADS_DEV, HEAD, D)
    wk_dev = jnp.repeat(jnp.transpose(w_k, (1, 0, 2)), REPL, axis=0)
    wv_dev = jnp.repeat(jnp.transpose(w_v, (1, 0, 2)), REPL, axis=0)

    def device_step(dx_acc, weights):
        wq_loc, wo_loc, wk_loc, wv_loc = weights
        wq_wide = wq_loc.astype(f32)
        wk_wide = wk_loc.astype(f32)
        wv_wide = wv_loc.astype(f32)
        queries = jnp.einsum("tc,che->hte", x_wide, wq_wide).astype(bf16)
        key_rows = jnp.dot(x_in, wk_loc, preferred_element_type=f32).astype(bf16)
        val_rows = jnp.dot(x_in, wv_loc, preferred_element_type=f32).astype(bf16)
        scores = jnp.einsum("hqe,ke->hqk", queries.astype(f32), key_rows.astype(f32)) * SCALE
        scores = jnp.where(causal, scores, -jnp.inf)
        attn_prob = jax.nn.softmax(scores, axis=-1)
        prob_bf = attn_prob.astype(bf16)
        attn_out = jnp.einsum("hqk,ke->hqe", prob_bf.astype(f32), val_rows.astype(f32)).astype(bf16)
        d_out = jnp.einsum("tc,hec->hte", dy_wide, wo_loc.astype(f32)).astype(bf16)
        grad_wo = jnp.einsum("hte,tc->hec", attn_out.astype(f32), dy_wide)
        d_prob = jnp.einsum("hqe,ke->hqk", d_out.astype(f32), val_rows.astype(f32))
        delta_row = jnp.sum(d_out.astype(f32) * attn_out.astype(f32), axis=-1, keepdims=True)
        d_score = (attn_prob * (d_prob - delta_row)).astype(bf16)
        d_query = (jnp.einsum("hqk,ke->hqe", d_score.astype(f32), key_rows.astype(f32)) * SCALE).astype(bf16)
        d_key = (jnp.einsum("hqk,hqe->ke", d_score.astype(f32), queries.astype(f32)) * SCALE).astype(bf16)
        d_val = jnp.einsum("hqk,hqe->ke", prob_bf.astype(f32), d_out.astype(f32)).astype(bf16)
        grad_wq = jnp.einsum("tc,hte->che", x_wide, d_query.astype(f32))
        dx_part = (jnp.einsum("hte,che->tc", d_query.astype(f32), wq_wide)
                   + jnp.dot(d_key.astype(f32), wk_wide.T)
                   + jnp.dot(d_val.astype(f32), wv_wide.T))
        return dx_acc + dx_part, (grad_wq, grad_wo, d_key, d_val)

    dx_sum, stacked = lax.scan(device_step, jnp.zeros((TOKENS, D), f32), (wq_dev, wo_dev, wk_dev, wv_dev))
    grad_wq, grad_wo, d_key, d_val = stacked
    dx_out = dx_sum.astype(bf16)
    dw_q = jnp.transpose(grad_wq, (1, 0, 2, 3)).reshape(D, HEADS, HEAD)
    dw_o = grad_wo.reshape(HEADS, HEAD, D)
    key_grp = d_key.reshape(KV_HEADS, REPL, TOKENS, HEAD).astype(f32)
    val_grp = d_val.reshape(KV_HEADS, REPL, TOKENS, HEAD).astype(f32)
    dw_k = jnp.einsum("tc,jrte->jce", x_wide, key_grp).reshape(KV_HEADS * D, HEAD)
    dw_v = jnp.einsum("tc,jrte->jce", x_wide, val_grp).reshape(KV_HEADS * D, HEAD)
    return dx_out, dw_q, dw_o, dw_k, dw_v
```

```python
import functools

import jax
import jax.numpy as jnp
from jax import lax
from jax.experimental import pallas as pl
from jax.experimental.pallas import tpu as pltpu
from jax.sharding import PartitionSpec as P

MESH = pl.DeviceIdType.MESH
F32 = jnp.float32
BF16 = jnp.bfloat16
ANY = pl.BlockSpec(memory_space=pl.ANY)
VM = pl.BlockSpec(memory_space=pltpu.VMEM)
BLK = 128
HALF = 64
CHUNK = 256
X_NBR, Y_NBR, SIB = 2, 4, 1


def mm(a, b, ca, cb):
    return lax.dot_general(a, b, (((ca,), (cb,)), ((), ())), preferred_element_type=F32)


def rows_of(chunk):
    return pl.ds(pl.multiple_of(chunk * CHUNK, CHUNK), CHUNK)


def attend_chunk(chunk, n_heads, scale, q_ref, do_ref, k_ref, v_ref, put, dk_ref, dv_ref):
    for last in range(q_ref.shape[0] // CHUNK):

        @pl.when(chunk == last)
        def _(last=last):
            span = (last + 1) * CHUNK
            rows = pl.ds(last * CHUNK, CHUNK)

            def head(h, carry):
                cols = pl.ds(pl.multiple_of(h * BLK, BLK), BLK)
                q = q_ref[rows, cols]
                d_out = do_ref[rows, cols]
                keys = k_ref[:span, :]
                vals = v_ref[:span, :]
                s = mm(q, keys, 1, 1) * scale
                row = lax.broadcasted_iota(jnp.int32, (CHUNK, CHUNK), 0)
                col = lax.broadcasted_iota(jnp.int32, (CHUNK, CHUNK), 1)
                s_diag = jnp.where(row >= col, s[:, span - CHUNK :], -jnp.inf)
                s = s_diag if last == 0 else jnp.concatenate([s[:, : span - CHUNK], s_diag], axis=1)
                e = jnp.exp(s - jnp.max(s, axis=1, keepdims=True))
                p = e * (1.0 / jnp.sum(e, axis=1, keepdims=True))
                pb = p.astype(BF16)
                o = mm(pb, vals, 1, 0).astype(BF16)
                delta = jnp.sum(d_out.astype(F32) * o.astype(F32), axis=1, keepdims=True)
                ds = (p * (mm(d_out, vals, 1, 1) - delta)).astype(BF16)
                dq = (mm(ds, keys, 1, 0) * scale).astype(BF16)
                put(h, o, dq)
                dk_ref[:span, :] += mm(ds, q, 0, 0)
                dv_ref[:span, :] += mm(pb, d_out, 0, 0)
                return carry

            lax.fori_loop(0, n_heads, head, 0)


def gather_kernel(
    n_heads, scale,
    x_ref, dy_ref, wq_ref, wk_ref, wv_ref, wo_ref,
    xf_ref, dyf_ref, wqs_ref, q_ref, k_ref, v_ref, do_ref, dqm_ref, dqs_ref, o_ref, dk_ref, dv_ref,
    xb, yb, wq, wkv, wo, dq_tmp, send_sem, recv_sem, wsend, wrecv, lsem, osem,
):
    me = lax.axis_index("tp")
    chip = me // 2
    core = lax.rem(me, 2)
    partner = {m: jnp.bitwise_xor(me, m) for m in range(1, 8)}
    barrier = pltpu.get_barrier_semaphore()
    for m in (SIB, X_NBR, Y_NBR):
        pl.semaphore_signal(barrier, inc=1, device_id={"tp": partner[m]}, device_id_type=MESH)
    pl.semaphore_wait(barrier, 3)

    bufs = (xb, yb)
    srcs = (x_ref, dy_ref)
    outs = (xf_ref, dyf_ref)
    counts = [0, 0]
    sends = []

    def part(t, block, half):
        return bufs[t].at[block, pl.ds(half * HALF, HALF)]

    def send(t, block, half, mask, own=False):
        src = srcs[t].at[pl.ds(half * HALF, HALF)] if own else part(t, block, half)
        copy = pltpu.make_async_remote_copy(
            src_ref=src,
            dst_ref=part(t, block, half),
            send_sem=send_sem.at[t, counts[t]],
            recv_sem=recv_sem.at[t, block, half],
            device_id={"tp": partner[mask]},
            device_id_type=MESH,
        )
        counts[t] += 1
        copy.start()
        sends.append(copy)

    def arrive(t, mask, half):
        block = partner[mask]
        pltpu.make_async_remote_copy(
            src_ref=part(t, block, half),
            dst_ref=part(t, block, half),
            send_sem=send_sem.at[t, 0],
            recv_sem=recv_sem.at[t, block, half],
            device_id={"tp": partner[SIB]},
            device_id_type=MESH,
        ).wait_recv()

    for half in range(2):
        send(0, me, half, X_NBR, own=True)
        send(0, me, half, Y_NBR, own=True)
    send(1, me, 0, X_NBR, own=True)
    send(1, me, 1, Y_NBR, own=True)
    loads = [
        pltpu.make_async_copy(x_ref, xb.at[me], lsem.at[0]),
        pltpu.make_async_copy(wq_ref, wq, lsem.at[1]),
        pltpu.make_async_copy(wk_ref, wkv.at[0], lsem.at[2]),
        pltpu.make_async_copy(wv_ref, wkv.at[1], lsem.at[3]),
        pltpu.make_async_copy(dy_ref, yb.at[me], lsem.at[4]),
        pltpu.make_async_copy(wo_ref, wo, lsem.at[5]),
    ]
    for copy in loads:
        copy.start()
    for half in range(2):
        send(0, me, half, SIB, own=True)
    for half in range(2):
        send(1, me, half, SIB, own=True)
    w_copy = pltpu.make_async_remote_copy(
        src_ref=wq_ref, dst_ref=wqs_ref, send_sem=wsend, recv_sem=wrecv,
        device_id={"tp": partner[SIB]}, device_id_type=MESH,
    )
    w_copy.start()
    dk_ref[...] = jnp.zeros_like(dk_ref)
    dv_ref[...] = jnp.zeros_like(dv_ref)

    writes = []

    def chunk_of(p):
        return jnp.bitwise_xor(chip, p)

    def write_out(t, p):
        chunk = chunk_of(p)
        for i in range(2):
            copy = pltpu.make_async_copy(
                bufs[t].at[2 * chunk + i],
                outs[t].at[pl.ds(pl.multiple_of((2 * chunk + i) * BLK, BLK), BLK)],
                osem.at[t, p, i],
            )
            copy.start()
            writes.append(copy)

    def project(p):
        chunk = chunk_of(p)
        rows = rows_of(chunk)
        x = xb[pl.ds(2 * chunk, 2)].reshape(CHUNK, xb.shape[2])

        def pair(j, carry):
            w = jnp.concatenate([wq[2 * j], wq[2 * j + 1]], axis=1)
            q_ref[rows, pl.ds(pl.multiple_of(j * 2 * BLK, 2 * BLK), 2 * BLK)] = mm(x, w, 1, 0).astype(BF16)
            return carry

        lax.fori_loop(0, n_heads // 2, pair, 0)
        kv = mm(x, jnp.concatenate([wkv[0], wkv[1]], axis=1), 1, 0).astype(BF16)
        k_ref[rows, :] = kv[:, :BLK]
        v_ref[rows, :] = kv[:, BLK:]
        write_out(0, p)

    def project_out(p):
        chunk = chunk_of(p)
        rows = rows_of(chunk)
        y = yb[pl.ds(2 * chunk, 2)].reshape(CHUNK, yb.shape[2])

        def pair(j, carry):
            w = wo[pl.ds(2 * j, 2)].reshape(2 * BLK, wo.shape[2])
            do_ref[rows, pl.ds(pl.multiple_of(j * 2 * BLK, 2 * BLK), 2 * BLK)] = mm(y, w, 1, 1).astype(BF16)
            return carry

        lax.fori_loop(0, n_heads // 2, pair, 0)
        write_out(1, p)

    def both(t, mask):
        arrive(t, mask, 0)
        arrive(t, mask, 1)

    for copy in loads[:4]:
        copy.wait()
    both(0, SIB)
    project(0)
    for copy in loads[4:]:
        copy.wait()
    both(1, SIB)
    project_out(0)
    arrive(0, X_NBR, 0)
    send(0, partner[X_NBR], 0, Y_NBR)
    arrive(0, Y_NBR, 1)
    send(0, partner[Y_NBR], 1, X_NBR)
    send(0, partner[X_NBR], 0, SIB)
    send(0, partner[Y_NBR], 1, SIB)
    arrive(0, X_NBR, 1)
    send(0, partner[X_NBR], 1, SIB)
    arrive(0, Y_NBR, 0)
    send(0, partner[Y_NBR], 0, SIB)
    both(0, X_NBR ^ SIB)
    project(1)
    both(0, Y_NBR ^ SIB)
    project(2)
    arrive(1, X_NBR, 0)
    send(1, partner[X_NBR], 0, Y_NBR)
    arrive(1, Y_NBR, 1)
    send(1, partner[Y_NBR], 1, X_NBR)
    send(1, me, 1, X_NBR, own=True)
    send(1, me, 0, Y_NBR, own=True)
    send(1, partner[X_NBR], 0, SIB)
    send(1, partner[Y_NBR], 1, SIB)
    diag = X_NBR ^ Y_NBR
    for t in range(2):
        for half in range(2):
            arrive(t, diag, half)
            send(t, partner[diag], half, SIB)
        both(t, diag ^ SIB)
        if t == 0:
            project(3)
        else:
            project_out(3)

    chunk_d = chunk_of(3)

    def put(h, o, dq):
        cols = pl.ds(pl.multiple_of(h * BLK, BLK), BLK)
        o_ref[:, cols] = o
        dq_tmp[0, :, cols] = dq[:BLK]
        dq_tmp[1, :, cols] = dq[BLK:]

    attend_chunk(chunk_d, n_heads, scale, q_ref, do_ref, k_ref, v_ref, put, dk_ref, dv_ref)
    dqm_ref[...] = dq_tmp[core]
    dqs_ref[...] = dq_tmp[1 - core]
    arrive(1, X_NBR, 1)
    send(1, partner[X_NBR], 1, SIB)
    arrive(1, Y_NBR, 0)
    send(1, partner[Y_NBR], 0, SIB)
    both(1, X_NBR ^ SIB)
    project_out(1)
    both(1, Y_NBR ^ SIB)
    project_out(2)
    for copy in sends:
        copy.wait_send()
    w_copy.wait()
    for copy in writes:
        copy.wait()


def gather_project(x_blk, dy_blk, wq, wk, wv, wo, n_dev, scale):
    n_heads, dim, hd = wq.shape
    tokens = x_blk.shape[0] * n_dev
    wide = n_heads * hd
    sds = jax.ShapeDtypeStruct
    return pl.pallas_call(
        functools.partial(gather_kernel, n_heads, scale),
        out_shape=(
            sds((tokens, dim), BF16), sds((tokens, dim), BF16), sds(wq.shape, BF16),
            sds((tokens, wide), BF16), sds((tokens, hd), BF16), sds((tokens, hd), BF16), sds((tokens, wide), BF16),
            sds((BLK, wide), BF16), sds((BLK, wide), BF16), sds((CHUNK, wide), BF16),
            sds((tokens, hd), F32), sds((tokens, hd), F32),
        ),
        in_specs=[ANY] * 6,
        out_specs=(ANY,) * 3 + (VM,) * 9,
        scratch_shapes=[
            pltpu.VMEM((n_dev, BLK, dim), BF16),
            pltpu.VMEM((n_dev, BLK, dim), BF16),
            pltpu.VMEM(wq.shape, BF16),
            pltpu.VMEM((2, dim, hd), BF16),
            pltpu.VMEM(wo.shape, BF16),
            pltpu.VMEM((2, BLK, wide), BF16),
            pltpu.SemaphoreType.DMA((2, 14)),
            pltpu.SemaphoreType.DMA((2, n_dev, 2)),
            pltpu.SemaphoreType.DMA,
            pltpu.SemaphoreType.DMA,
            pltpu.SemaphoreType.DMA((6,)),
            pltpu.SemaphoreType.DMA((2, 4, 2)),
        ],
        compiler_params=pltpu.CompilerParams(
            collective_id=0, has_side_effects=True, vmem_limit_bytes=67043328
        ),
        name="gather_project",
    )(x_blk, dy_blk, wq, wk, wv, wo)


def attend_kernel(
    n_heads, scale,
    q_ref, k_ref, v_ref, do_ref, od_ref, dqd_ref, dqs_ref, dk0_ref, dv0_ref,
    o_ref, dq_ref, mine_ref, give_ref, dk_ref, dv_ref,
):
    me = lax.axis_index("tp")
    chip = me // 2
    core = lax.rem(me, 2)
    wide = q_ref.shape[1]
    dk_ref[...] = dk0_ref[...]
    dv_ref[...] = dv0_ref[...]

    def step(i, carry):
        chunk = jnp.bitwise_xor(chip, lax.rem(i + 1, 3))
        rows = rows_of(chunk)

        def put(h, o, dq):
            cols = pl.ds(pl.multiple_of(h * BLK, BLK), BLK)
            o_ref[rows, cols] = o
            dq_ref[rows, cols] = dq

        attend_chunk(chunk, n_heads, scale, q_ref, do_ref, k_ref, v_ref, put, dk_ref, dv_ref)
        return carry

    lax.fori_loop(0, 3, step, 0)
    chunk_d = jnp.bitwise_xor(chip, 3)
    o_ref[rows_of(chunk_d), :] = od_ref[...]
    dq_ref[pl.ds(pl.multiple_of(chunk_d * CHUNK + core * BLK, BLK), BLK), :] = dqd_ref[...]
    dq_ref[pl.ds(pl.multiple_of(chunk_d * CHUNK + (1 - core) * BLK, BLK), BLK), :] = dqs_ref[...]
    for p in range(4):
        chunk = jnp.bitwise_xor(chip, p)
        for ref, cls in ((mine_ref, core), (give_ref, 1 - core)):
            rows = pl.ds(pl.multiple_of(chunk * CHUNK + cls * BLK, BLK), BLK)
            ref[p, :, :wide] = dq_ref[rows, :]
            ref[p, :, wide : wide + BLK] = (dk_ref[rows, :] * scale).astype(BF16)
            ref[p, :, wide + BLK :] = dv_ref[rows, :].astype(BF16)


def attend(q, k, v, d_out, o_d, dqm_d, dqs_d, dk0, dv0, n_heads, scale):
    tokens, wide = q.shape
    hd = k.shape[1]
    sds = jax.ShapeDtypeStruct
    pairs = tokens * tokens * n_heads // 2
    return pl.pallas_call(
        functools.partial(attend_kernel, n_heads, scale),
        out_shape=(
            sds((tokens, wide), BF16), sds((tokens, wide), BF16),
            sds((4, BLK, wide + 2 * hd), BF16), sds((4, BLK, wide + 2 * hd), BF16),
        ),
        in_specs=[VM] * 9,
        out_specs=(VM,) * 4,
        scratch_shapes=[pltpu.VMEM((tokens, hd), F32), pltpu.VMEM((tokens, hd), F32)],
        compiler_params=pltpu.CompilerParams(vmem_limit_bytes=48 * 2**20),
        cost_estimate=pl.CostEstimate(flops=pairs * hd * 24, bytes_accessed=12 * 2**20, transcendentals=pairs),
        name="attend",
    )(q, k, v, d_out, o_d, dqm_d, dqs_d, dk0, dv0)


def dx_kernel(groups, wide, mine_ref, got_ref, wa_ref, wb_ref, sa_ref, sb_ref, *out_refs):
    lhs = jnp.concatenate(
        [
            jnp.concatenate([mine_ref[g, :, :wide] for g in groups], axis=0),
            jnp.concatenate([got_ref[g, :, :wide] for g in groups], axis=0),
        ],
        axis=1,
    )
    for side, (w_ref, s_ref) in enumerate(((wa_ref, sa_ref), (wb_ref, sb_ref))):
        n = w_ref.shape[0]
        rhs = jnp.concatenate([w_ref[h] for h in range(n)] + [s_ref[h] for h in range(n)], axis=1)
        res = mm(lhs, rhs, 1, 1)
        for i in range(len(groups)):
            out_refs[2 * i + side][...] = res[i * BLK : (i + 1) * BLK]


def dx_partial(mine, got, wq, wqs, groups):
    n_heads, dim, hd = wq.shape
    tile = 512
    half = dim // 2
    steps = half // tile
    rows = BLK * len(groups)
    w_lo = pl.BlockSpec((n_heads, tile, hd), lambda j: (0, j, 0))
    w_hi = pl.BlockSpec((n_heads, tile, hd), lambda j: (0, j + steps, 0))
    whole = pl.BlockSpec(mine.shape, lambda j: (0, 0, 0))
    return pl.pallas_call(
        functools.partial(dx_kernel, groups, n_heads * hd),
        grid=(steps,),
        out_shape=(jax.ShapeDtypeStruct((BLK, half), F32),) * (2 * len(groups)),
        in_specs=[whole, whole, w_lo, w_hi, w_lo, w_hi],
        out_specs=(pl.BlockSpec((BLK, tile), lambda j: (0, j)),) * (2 * len(groups)),
        compiler_params=pltpu.CompilerParams(vmem_limit_bytes=40 * 2**20),
        cost_estimate=pl.CostEstimate(
            flops=4 * rows * dim * n_heads * hd, bytes_accessed=4 * dim * n_heads * hd + 4 * rows * dim, transcendentals=0
        ),
        name="dx_partial",
    )(mine, got, wq, wq, wqs, wqs)


def dwo_kernel(o_ref, dy_ref, out_ref, o_t):
    @pl.when(pl.program_id(0) == 0)
    def _():
        o_t[...] = o_ref[...].T

    res = mm(o_t[...], dy_ref[...], 1, 0)
    for h in range(out_ref.shape[0]):
        out_ref[h] = res[h * BLK : (h + 1) * BLK]


def grad_wo(o, dy_full):
    tokens, wide = o.shape
    dim = dy_full.shape[1]
    tile = 512
    n_heads = wide // BLK
    return pl.pallas_call(
        dwo_kernel,
        grid=(dim // tile,),
        out_shape=jax.ShapeDtypeStruct((n_heads, BLK, dim), F32),
        in_specs=[pl.BlockSpec((tokens, wide), lambda j: (0, 0)), pl.BlockSpec((tokens, tile), lambda j: (0, j))],
        out_specs=pl.BlockSpec((n_heads, BLK, tile), lambda j: (0, 0, j)),
        scratch_shapes=[pltpu.VMEM((wide, tokens), BF16)],
        compiler_params=pltpu.CompilerParams(vmem_limit_bytes=40 * 2**20),
        cost_estimate=pl.CostEstimate(
            flops=2 * tokens * wide * dim, bytes_accessed=2 * tokens * dim + 4 * wide * dim, transcendentals=0
        ),
        name="grad_wo",
    )(o, dy_full)


def dwq_kernel(x_ref, dq_ref, out_ref):
    res = mm(x_ref[...], dq_ref[...], 0, 0)
    for h in range(out_ref.shape[0]):
        out_ref[h] = res[:, h * BLK : (h + 1) * BLK]


def grad_wq(x_full, dq):
    tokens, wide = dq.shape
    dim = x_full.shape[1]
    tile = 512
    n_heads = wide // BLK
    return pl.pallas_call(
        dwq_kernel,
        grid=(dim // tile,),
        out_shape=jax.ShapeDtypeStruct((n_heads, dim, BLK), F32),
        in_specs=[pl.BlockSpec((tokens, tile), lambda j: (0, j)), pl.BlockSpec((tokens, wide), lambda j: (0, 0))],
        out_specs=pl.BlockSpec((n_heads, tile, BLK), lambda j: (0, j, 0)),
        compiler_params=pltpu.CompilerParams(vmem_limit_bytes=40 * 2**20),
        cost_estimate=pl.CostEstimate(
            flops=2 * tokens * wide * dim, bytes_accessed=2 * tokens * dim + 4 * wide * dim, transcendentals=0
        ),
        name="grad_wq",
    )(x_full, dq)


def split3(a):
    hi = a.astype(BF16)
    rest = a - hi.astype(F32)
    mid = rest.astype(BF16)
    low = (rest - mid.astype(F32)).astype(BF16)
    return hi, mid, low


def kv_kernel(me_ref, mine_ref, other_ref, x_ref, dwk_ref, dwv_ref, rows_ref):
    me = me_ref[0]
    chip = me // 2
    core = lax.rem(me, 2)
    wide = mine_ref.shape[2]
    for p in range(4):
        chunk = jnp.bitwise_xor(chip, p)
        for ref, cls in ((mine_ref, core), (other_ref, 1 - core)):
            rows = pl.ds(pl.multiple_of(chunk * CHUNK + cls * BLK, BLK), BLK)
            for i, piece in enumerate(split3(ref[p])):
                rows_ref[rows, i * wide : (i + 1) * wide] = piece
    res = mm(x_ref[...], rows_ref[...], 0, 0)
    res = res[:, :wide] + res[:, wide : 2 * wide] + res[:, 2 * wide :]
    dwk_ref[...] = res[:, :BLK]
    dwv_ref[...] = res[:, BLK:]


def grad_kv(me, mine, other, x_full, n_dev):
    tokens, dim = x_full.shape
    own = dim // n_dev
    whole = pl.BlockSpec(mine.shape, lambda i, m: (0, 0, 0))
    out = pl.BlockSpec((own, BLK), lambda i, m: (0, 0))
    return pl.pallas_call(
        kv_kernel,
        grid_spec=pltpu.PrefetchScalarGridSpec(
            num_scalar_prefetch=1,
            grid=(1,),
            in_specs=[whole, whole, pl.BlockSpec((tokens, own), lambda i, m: (0, m[0]))],
            out_specs=(out, out),
            scratch_shapes=[pltpu.VMEM((tokens, 3 * mine.shape[2]), BF16)],
        ),
        out_shape=(jax.ShapeDtypeStruct((own, BLK), F32),) * 2,
        compiler_params=pltpu.CompilerParams(vmem_limit_bytes=40 * 2**20),
        cost_estimate=pl.CostEstimate(
            flops=2 * tokens * own * 3 * mine.shape[2], bytes_accessed=4 * tokens * own, transcendentals=0
        ),
        name="grad_kv",
    )(me, mine, other, x_full)


def kvdx_kernel(sum_ref, wka_ref, wkb_ref, wva_ref, wvb_ref, pa_ref, pb_ref, oa_ref, ob_ref):
    pieces = split3(sum_ref[0])
    for wk_ref, wv_ref, p_ref, o_ref in (
        (wka_ref, wva_ref, pa_ref, oa_ref),
        (wkb_ref, wvb_ref, pb_ref, ob_ref),
    ):
        w = jnp.concatenate([wk_ref[...], wv_ref[...]], axis=1)
        res = mm(jnp.concatenate(pieces, axis=0), w, 1, 1)
        o_ref[...] = p_ref[...] + (res[:BLK] + res[BLK : 2 * BLK] + res[2 * BLK :])


def kv_dx(total, wk, wv, pa, pb):
    dim, hd = wk.shape
    half = dim // 2
    tile = 1024
    steps = half // tile
    w_lo = pl.BlockSpec((tile, hd), lambda j: (j, 0))
    w_hi = pl.BlockSpec((tile, hd), lambda j: (j + steps, 0))
    col = pl.BlockSpec((BLK, tile), lambda j: (0, j))
    return pl.pallas_call(
        kvdx_kernel,
        grid=(steps,),
        out_shape=(jax.ShapeDtypeStruct((BLK, half), F32),) * 2,
        in_specs=[pl.BlockSpec((1,) + total.shape[1:], lambda j: (0, 0, 0)), w_lo, w_hi, w_lo, w_hi, col, col],
        out_specs=(col, col),
        compiler_params=pltpu.CompilerParams(vmem_limit_bytes=40 * 2**20),
        cost_estimate=pl.CostEstimate(flops=12 * BLK * dim * hd, bytes_accessed=10 * 2**20, transcendentals=0),
        name="kv_dx",
    )(total, wk, wk, wv, wv, pa, pb)


def solution(mesh):
    n_dev = mesh.shape["tp"]

    def swap(a, mask):
        return lax.ppermute(a, "tp", [(i, i ^ mask) for i in range(n_dev)])

    def local_grads(x_blk, dy_blk, wq_loc, w_k, w_v, wo_loc):
        n_heads, hd = wq_loc.shape[1:]
        scale = hd ** -0.5
        wide = n_heads * hd
        wq = jnp.transpose(wq_loc, (1, 0, 2))
        wk = w_k[:, 0, :]
        wv = w_v[:, 0, :]
        me = lax.axis_index("tp").astype(jnp.int32).reshape(1)
        xf, dyf, wqs, q, k, v, d_out, dqm_d, dqs_d, o_d, dk0, dv0 = gather_project(
            x_blk, dy_blk, wq, wk, wv, wo_loc, n_dev, scale
        )
        dqg_d = swap(dqs_d, SIB)
        pd_a, pd_b = dx_partial(dqm_d[None], dqg_d[None], wq, wqs, (0,))
        ra = swap(pd_a, X_NBR)
        rb = swap(pd_b, Y_NBR)
        o, dq, mine, give = attend(q, k, v, d_out, o_d, dqm_d, dqs_d, dk0, dv0, n_heads, scale)
        got = swap(give, SIB)
        kvs = mine[:, :, wide:].astype(F32) + got[:, :, wide:].astype(F32)
        kv_x = swap(kvs, X_NBR)
        kv_y = swap(kvs, Y_NBR)
        px_a, px_b, py_a, py_b, po_a, po_b = dx_partial(mine, got, wq, wqs, (1, 2, 0))
        a2 = swap(px_a, X_NBR)
        b2 = swap(py_b, Y_NBR)
        kv_d = jnp.concatenate([swap(kv_x[:2], Y_NBR), swap(kv_y[2:], X_NBR)], axis=0)
        dwo = grad_wo(o, dyf)
        a3 = swap(py_a + ra, Y_NBR)
        b3 = swap(px_b + rb, X_NBR)
        total = jnp.stack([kvs[p] + kv_x[p ^ 1] + kv_y[p ^ 2] + kv_d[p ^ 3] for p in range(4)])
        other = swap(total, SIB)
        dwq = grad_wq(xf, dq)
        base_a, base_b = kv_dx(total, wk, wv, po_a, po_b)
        dwk, dwv = grad_kv(me, total, other, xf, n_dev)
        dx = jnp.concatenate([(base_a + a2) + a3, (base_b + b2) + b3], axis=1).astype(BF16)
        return dx, jnp.transpose(dwq, (1, 0, 2)), dwo, dwk, dwv

    tok_spec = P(("dp", "tp"))
    return jax.shard_map(
        local_grads,
        mesh=mesh,
        in_specs=(tok_spec, tok_spec, P(None, "tp", None), P(), P(), P("tp")),
        out_specs=(tok_spec, P("dp", "tp", None), tok_spec, tok_spec, tok_spec),
        check_vma=False,
    )
```

```python
import functools

import jax
import jax.numpy as jnp
from jax import lax
from jax.experimental import pallas as pl
from jax.experimental.pallas import tpu as pltpu
from jax.sharding import PartitionSpec as P

MESH = pl.DeviceIdType.MESH
F32 = jnp.float32
BF16 = jnp.bfloat16
ANY = pl.BlockSpec(memory_space=pl.ANY)
VM = pl.BlockSpec(memory_space=pltpu.VMEM)
BLK = 128
HALF = 64
FULL = 67043328
CHUNK = 256
X_NBR, Y_NBR, SIB = 2, 4, 1


def mm(a, b, ca, cb):
    return lax.dot_general(a, b, (((ca,), (cb,)), ((), ())), preferred_element_type=F32)


def rows_of(chunk):
    return pl.ds(pl.multiple_of(chunk * CHUNK, CHUNK), CHUNK)


def attend_chunk(chunk, n_heads, scale, q_ref, do_ref, k_ref, v_ref, put, dk_ref, dv_ref):
    for last in range(q_ref.shape[0] // CHUNK):

        @pl.when(chunk == last)
        def _(last=last):
            span = (last + 1) * CHUNK
            rows = pl.ds(last * CHUNK, CHUNK)

            def head(h, carry):
                cols = pl.ds(pl.multiple_of(h * BLK, BLK), BLK)
                q = q_ref[rows, cols]
                d_out = do_ref[rows, cols]
                keys = k_ref[:span, :]
                vals = v_ref[:span, :]
                s = mm(q, keys, 1, 1) * scale
                row = lax.broadcasted_iota(jnp.int32, (CHUNK, CHUNK), 0)
                col = lax.broadcasted_iota(jnp.int32, (CHUNK, CHUNK), 1)
                s_diag = jnp.where(row >= col, s[:, span - CHUNK :], -jnp.inf)
                s = s_diag if last == 0 else jnp.concatenate([s[:, : span - CHUNK], s_diag], axis=1)
                e = jnp.exp(s - jnp.max(s, axis=1, keepdims=True))
                p = e * (1.0 / jnp.sum(e, axis=1, keepdims=True))
                pb = p.astype(BF16)
                o = mm(pb, vals, 1, 0).astype(BF16)
                delta = jnp.sum(d_out.astype(F32) * o.astype(F32), axis=1, keepdims=True)
                ds = (p * (mm(d_out, vals, 1, 1) - delta)).astype(BF16)
                dq = (mm(ds, keys, 1, 0) * scale).astype(BF16)
                put(h, o, dq)
                dk_ref[:span, :] += mm(ds, q, 0, 0)
                dv_ref[:span, :] += mm(pb, d_out, 0, 0)
                return carry

            lax.fori_loop(0, n_heads, head, 0)


def front_kernel(
    n_heads, scale,
    x_ref, dy_ref, wq_ref, wk_ref, wv_ref, wo_ref,
    xf_ref, dyf_ref, wqs_ref, pd_ref, r_ref, pxa_ref, pxb_ref, pya_ref, pyb_ref, poa_ref, pob_ref,
    of_ref, dqf_ref, kvo_ref, kx0_ref, kx1_ref, ky0_ref, ky1_ref,
    xb, yb, wq, wkv, wo, q_ref, do_ref, o_ref, dq_ref, k_ref, v_ref, dk_ref, dv_ref,
    wt, pt, rt, got_q, dkv, got_kv, kvs,
    send_sem, recv_sem, wsem, lsem, osem, gq_send, gq_recv, gkv_send, gkv_recv,
    r_send, r_recv, kn_send, kn_recv, wt_sem, pt_sem, rt_sem, att_sem,
):
    me = lax.axis_index("tp")
    chip = me // 2
    core = lax.rem(me, 2)
    partner = {m: jnp.bitwise_xor(me, m) for m in range(1, 8)}
    barrier = pltpu.get_barrier_semaphore()
    for m in (SIB, X_NBR, Y_NBR):
        pl.semaphore_signal(barrier, inc=1, device_id={"tp": partner[m]}, device_id_type=MESH)
    pl.semaphore_wait(barrier, 3)

    bufs = (xb, yb)
    srcs = (x_ref, dy_ref)
    outs = (xf_ref, dyf_ref)
    counts = [0, 0]
    sends = []

    def remote(src, dst, ssem, rsem, mask):
        return pltpu.make_async_remote_copy(
            src_ref=src, dst_ref=dst, send_sem=ssem, recv_sem=rsem,
            device_id={"tp": partner[mask]}, device_id_type=MESH,
        )

    def part(t, block, half):
        return bufs[t].at[block, pl.ds(half * HALF, HALF)]

    def send(t, block, half, mask, own=False):
        src = srcs[t].at[pl.ds(half * HALF, HALF)] if own else part(t, block, half)
        copy = remote(src, part(t, block, half), send_sem.at[t, counts[t]], recv_sem.at[t, block, half], mask)
        counts[t] += 1
        copy.start()
        sends.append(copy)

    def arrive(t, mask, half):
        block = partner[mask]
        here = part(t, block, half)
        remote(here, here, send_sem.at[t, 0], recv_sem.at[t, block, half], SIB).wait_recv()

    for half in range(2):
        send(0, me, half, X_NBR, own=True)
        send(0, me, half, Y_NBR, own=True)
    send(1, me, 0, X_NBR, own=True)
    send(1, me, 1, Y_NBR, own=True)
    loads = [
        pltpu.make_async_copy(x_ref, xb.at[me], lsem.at[0]),
        pltpu.make_async_copy(wq_ref, wq, lsem.at[1]),
        pltpu.make_async_copy(wk_ref, wkv.at[0], lsem.at[2]),
        pltpu.make_async_copy(wv_ref, wkv.at[1], lsem.at[3]),
        pltpu.make_async_copy(dy_ref, yb.at[me], lsem.at[4]),
        pltpu.make_async_copy(wo_ref, wo, lsem.at[5]),
    ]
    for copy in loads:
        copy.start()
    for half in range(2):
        send(0, me, half, SIB, own=True)
    for half in range(2):
        send(1, me, half, SIB, own=True)
    w_copy = remote(wq_ref, wqs_ref, wsem.at[0], wsem.at[1], SIB)
    w_copy.start()
    dk_ref[...] = jnp.zeros_like(dk_ref)
    dv_ref[...] = jnp.zeros_like(dv_ref)

    writes = []

    def chunk_of(p):
        return jnp.bitwise_xor(chip, p)

    def block_rows(p, cls):
        return pl.ds(pl.multiple_of(chunk_of(p) * CHUNK + cls * BLK, BLK), BLK)

    def write_out(t, p):
        chunk = chunk_of(p)
        for i in range(2):
            copy = pltpu.make_async_copy(
                bufs[t].at[2 * chunk + i],
                outs[t].at[pl.ds(pl.multiple_of((2 * chunk + i) * BLK, BLK), BLK)],
                osem.at[t, p, i],
            )
            copy.start()
            writes.append(copy)

    def project(p):
        chunk = chunk_of(p)
        rows = rows_of(chunk)
        x = xb[pl.ds(2 * chunk, 2)].reshape(CHUNK, xb.shape[2])

        def pair(j, carry):
            w = jnp.concatenate([wq[2 * j], wq[2 * j + 1]], axis=1)
            q_ref[rows, pl.ds(pl.multiple_of(j * 2 * BLK, 2 * BLK), 2 * BLK)] = mm(x, w, 1, 0).astype(BF16)
            return carry

        lax.fori_loop(0, n_heads // 2, pair, 0)
        kv = mm(x, jnp.concatenate([wkv[0], wkv[1]], axis=1), 1, 0).astype(BF16)
        k_ref[rows, :] = kv[:, :BLK]
        v_ref[rows, :] = kv[:, BLK:]
        write_out(0, p)

    def project_out(p):
        chunk = chunk_of(p)
        rows = rows_of(chunk)
        y = yb[pl.ds(2 * chunk, 2)].reshape(CHUNK, yb.shape[2])

        def pair(j, carry):
            w = wo[pl.ds(2 * j, 2)].reshape(2 * BLK, wo.shape[2])
            do_ref[rows, pl.ds(pl.multiple_of(j * 2 * BLK, 2 * BLK), 2 * BLK)] = mm(y, w, 1, 1).astype(BF16)
            return carry

        lax.fori_loop(0, n_heads // 2, pair, 0)
        write_out(1, p)

    def both(t, mask):
        arrive(t, mask, 0)
        arrive(t, mask, 1)

    def attend_rows(p):
        chunk = chunk_of(p)
        rows = rows_of(chunk)

        def put(h, o, dq):
            cols = pl.ds(pl.multiple_of(h * BLK, BLK), BLK)
            o_ref[rows, cols] = o
            dq_ref[rows, cols] = dq

        attend_chunk(chunk, n_heads, scale, q_ref, do_ref, k_ref, v_ref, put, dk_ref, dv_ref)

    def att_out(p):
        rows = rows_of(chunk_of(p))
        return (
            pltpu.make_async_copy(o_ref.at[rows], of_ref.at[rows], att_sem.at[p, 0]),
            pltpu.make_async_copy(dq_ref.at[rows], dqf_ref.at[rows], att_sem.at[p, 1]),
        )

    def give_q(p):
        return remote(dq_ref.at[block_rows(p, 1 - core)], got_q.at[p], gq_send.at[p], gq_recv.at[p], SIB)

    def give_kv(p):
        return remote(dkv.at[block_rows(p, 1 - core)], got_kv.at[p], gkv_send.at[p], gkv_recv.at[p], SIB)

    tile = wt.shape[2]
    steps = pd_ref.shape[1]

    def w_load(side, i):
        col = pl.multiple_of((side * steps + i) * tile, tile)
        return pltpu.make_async_copy(wqs_ref.at[:, pl.ds(col, tile), :], wt.at[side], wt_sem.at[side])

    def product(groups, side, i):
        col = pl.multiple_of((side * steps + i) * tile, tile)
        lhs = jnp.concatenate(
            [
                jnp.concatenate([dq_ref[block_rows(p, core), :] for p in groups], axis=0),
                jnp.concatenate([got_q[p] for p in groups], axis=0),
            ],
            axis=1,
        )
        rhs = jnp.concatenate(
            [wq[h, pl.ds(col, tile), :] for h in range(n_heads)] + [wt[side, h] for h in range(n_heads)], axis=1
        )
        return mm(lhs, rhs, 1, 1)

    for copy in loads[:4]:
        copy.wait()
    both(0, SIB)
    project(0)
    for copy in loads[4:]:
        copy.wait()
    both(1, SIB)
    project_out(0)
    arrive(0, X_NBR, 0)
    send(0, partner[X_NBR], 0, Y_NBR)
    arrive(0, Y_NBR, 1)
    send(0, partner[Y_NBR], 1, X_NBR)
    send(0, partner[X_NBR], 0, SIB)
    send(0, partner[Y_NBR], 1, SIB)
    arrive(0, X_NBR, 1)
    send(0, partner[X_NBR], 1, SIB)
    arrive(0, Y_NBR, 0)
    send(0, partner[Y_NBR], 0, SIB)
    both(0, X_NBR ^ SIB)
    project(1)
    both(0, Y_NBR ^ SIB)
    project(2)
    arrive(1, X_NBR, 0)
    send(1, partner[X_NBR], 0, Y_NBR)
    arrive(1, Y_NBR, 1)
    send(1, partner[Y_NBR], 1, X_NBR)
    send(1, me, 1, X_NBR, own=True)
    send(1, me, 0, Y_NBR, own=True)
    send(1, partner[X_NBR], 0, SIB)
    send(1, partner[Y_NBR], 1, SIB)
    diag = X_NBR ^ Y_NBR
    for t in range(2):
        for half in range(2):
            arrive(t, diag, half)
            send(t, partner[diag], half, SIB)
        both(t, diag ^ SIB)
        if t == 0:
            project(3)
        else:
            project_out(3)

    attend_rows(3)
    give_q(3).start()
    w_copy.wait()
    for side in range(2):
        w_load(side, 0).start()
    for copy in att_out(3):
        copy.start()
    give_q(3).wait_recv()

    def pd_write(side, i):
        return pltpu.make_async_copy(pt.at[side, pl.ds(0, BLK)], pd_ref.at[side, i], pt_sem.at[side, 0])

    def round1(side, i):
        mask = (X_NBR, Y_NBR)[side]
        return remote(pd_ref.at[side, i], r_ref.at[side, i], r_send.at[side, i], r_recv.at[side, i], mask)

    def pd_step(i, carry):
        for side in range(2):
            w_load(side, i).wait()
            res = product((3,), side, i)

            @pl.when(i > 0)
            def _(side=side):
                pd_write(side, i - 1).wait()
                round1(side, i - 1).start()

            pt[side, :BLK] = res
            pd_write(side, i).start()

            @pl.when(i < steps - 1)
            def _(side=side):
                w_load(side, i + 1).start()

        return carry

    lax.fori_loop(0, steps, pd_step, 0)
    for side in range(2):
        pd_write(side, steps - 1).wait()
        round1(side, steps - 1).start()
        w_load(side, 0).start()

    arrive(1, X_NBR, 1)
    send(1, partner[X_NBR], 1, SIB)
    arrive(1, Y_NBR, 0)
    send(1, partner[Y_NBR], 0, SIB)
    both(1, X_NBR ^ SIB)
    project_out(1)
    both(1, Y_NBR ^ SIB)
    project_out(2)

    def rest(i, carry):
        p = lax.rem(i + 1, 3)
        attend_rows(p)
        give_q(p).start()
        for copy in att_out(p):
            copy.start()
        return carry

    lax.fori_loop(0, 3, rest, 0)
    dkv[:, :BLK] = (dk_ref[...] * scale).astype(BF16)
    dkv[:, BLK:] = dv_ref[...].astype(BF16)
    for p in range(3):
        give_q(p).wait_recv()
    for p in range(4):
        give_kv(p).start()

    def r_load(side, i):
        return pltpu.make_async_copy(r_ref.at[side, i], rt.at[side], rt_sem.at[side])

    groups = (1, 2, 0)
    targets = ((pxa_ref, pya_ref, poa_ref), (pxb_ref, pyb_ref, pob_ref))

    def p_writes(side, i):
        return [
            pltpu.make_async_copy(pt.at[side, pl.ds(g * BLK, BLK)], targets[side][g].at[i], pt_sem.at[side, g])
            for g in range(3)
        ]

    def p_step(i, carry):
        for side in range(2):
            round1(side, i).wait_recv()
            r_load(side, i).start()
            w_load(side, i).wait()
            res = product(groups, side, i)

            @pl.when(i > 0)
            def _(side=side):
                for copy in p_writes(side, i - 1):
                    copy.wait()

            r_load(side, i).wait()
            add = 1 - side
            for g in range(3):
                rows = res[g * BLK : (g + 1) * BLK]
                pt[side, g * BLK : (g + 1) * BLK] = rows + rt[side] if g == add else rows
            for copy in p_writes(side, i):
                copy.start()

            @pl.when(i < steps - 1)
            def _(side=side):
                w_load(side, i + 1).start()

        return carry

    for p in range(4):
        give_kv(p).wait_recv()
        kvs[p] = dkv[block_rows(p, core), :].astype(F32) + got_kv[p].astype(F32)
    p_step(0, 0)
    near = [
        remote(kvs.at[pl.ds(2 * i, 2)], dst, kn_send.at[n, i], kn_recv.at[n, i], mask)
        for n, (mask, dsts) in enumerate(((X_NBR, (kx0_ref, kx1_ref)), (Y_NBR, (ky0_ref, ky1_ref))))
        for i, dst in enumerate(dsts)
    ]
    for copy in near:
        copy.start()
    kv_out = pltpu.make_async_copy(kvs, kvo_ref, lsem.at[0])
    kv_out.start()
    lax.fori_loop(1, steps, p_step, 0)
    for side in range(2):
        for copy in p_writes(side, steps - 1):
            copy.wait()
    for copy in sends:
        copy.wait_send()
    for p in range(4):
        give_q(p).wait_send()
        give_kv(p).wait_send()
        for copy in att_out(p):
            copy.wait()
    for side in range(2):
        for i in range(steps):
            round1(side, i).wait_send()
    for copy in near:
        copy.wait()
    kv_out.wait()
    for copy in writes:
        copy.wait()


TILE = 512


def front(x_blk, dy_blk, wq, wk, wv, wo, n_dev, scale):
    n_heads, dim, hd = wq.shape
    tokens = x_blk.shape[0] * n_dev
    wide = n_heads * hd
    steps = dim // 2 // TILE
    sds = jax.ShapeDtypeStruct
    sem = pltpu.SemaphoreType.DMA
    piece = sds((steps, BLK, TILE), F32)
    return pl.pallas_call(
        functools.partial(front_kernel, n_heads, scale),
        out_shape=(
            sds((tokens, dim), BF16), sds((tokens, dim), BF16), sds(wq.shape, BF16),
            sds((2, steps, BLK, TILE), F32), sds((2, steps, BLK, TILE), F32),
            piece, piece, piece, piece, piece, piece,
            sds((tokens, wide), BF16), sds((tokens, wide), BF16), sds((4, BLK, 2 * hd), F32),
        )
        + (sds((2, BLK, 2 * hd), F32),) * 4,
        in_specs=[ANY] * 6,
        out_specs=(ANY,) * 18,
        scratch_shapes=[
            pltpu.VMEM((n_dev, BLK, dim), BF16),
            pltpu.VMEM((n_dev, BLK, dim), BF16),
            pltpu.VMEM(wq.shape, BF16),
            pltpu.VMEM((2, dim, hd), BF16),
            pltpu.VMEM(wo.shape, BF16),
            pltpu.VMEM((tokens, wide), BF16),
            pltpu.VMEM((tokens, wide), BF16),
            pltpu.VMEM((tokens, wide), BF16),
            pltpu.VMEM((tokens, wide), BF16),
            pltpu.VMEM((tokens, hd), BF16),
            pltpu.VMEM((tokens, hd), BF16),
            pltpu.VMEM((tokens, hd), F32),
            pltpu.VMEM((tokens, hd), F32),
            pltpu.VMEM((2, n_heads, TILE, hd), BF16),
            pltpu.VMEM((2, 3 * BLK, TILE), F32),
            pltpu.VMEM((2, BLK, TILE), F32),
            pltpu.VMEM((4, BLK, wide), BF16),
            pltpu.VMEM((tokens, 2 * hd), BF16),
            pltpu.VMEM((4, BLK, 2 * hd), BF16),
            pltpu.VMEM((4, BLK, 2 * hd), F32),
            sem((2, 14)), sem((2, n_dev, 2)), sem((2,)), sem((6,)), sem((2, 4, 2)),
            sem((4,)), sem((4,)), sem((4,)), sem((4,)),
            sem((2, steps)), sem((2, steps)), sem((2, 2)), sem((2, 2)),
            sem((2,)), sem((2, 3)), sem((2,)), sem((4, 2)),
        ],
        compiler_params=pltpu.CompilerParams(collective_id=0, has_side_effects=True, vmem_limit_bytes=FULL),
        name="front",
    )(x_blk, dy_blk, wq, wk, wv, wo)


def dwo_kernel(o_ref, dy_ref, out_ref, o_t):
    @pl.when(pl.program_id(0) == 0)
    def _():
        o_t[...] = o_ref[...].T

    res = mm(o_t[...], dy_ref[...], 1, 0)
    for h in range(out_ref.shape[0]):
        out_ref[h] = res[h * BLK : (h + 1) * BLK]


def grad_wo(o, dy_full):
    tokens, wide = o.shape
    dim = dy_full.shape[1]
    tile = 512
    n_heads = wide // BLK
    return pl.pallas_call(
        dwo_kernel,
        grid=(dim // tile,),
        out_shape=jax.ShapeDtypeStruct((n_heads, BLK, dim), F32),
        in_specs=[pl.BlockSpec((tokens, wide), lambda j: (0, 0)), pl.BlockSpec((tokens, tile), lambda j: (0, j))],
        out_specs=pl.BlockSpec((n_heads, BLK, tile), lambda j: (0, 0, j)),
        scratch_shapes=[pltpu.VMEM((wide, tokens), BF16)],
        compiler_params=pltpu.CompilerParams(vmem_limit_bytes=FULL),
        cost_estimate=pl.CostEstimate(
            flops=2 * tokens * wide * dim, bytes_accessed=2 * tokens * dim + 4 * wide * dim, transcendentals=0
        ),
        name="grad_wo",
    )(o, dy_full)


def dwq_kernel(x_ref, dq_ref, out_ref):
    res = mm(x_ref[...], dq_ref[...], 0, 0)
    for h in range(out_ref.shape[0]):
        out_ref[h] = res[:, h * BLK : (h + 1) * BLK]


def grad_wq(x_full, dq):
    tokens, wide = dq.shape
    dim = x_full.shape[1]
    tile = 512
    n_heads = wide // BLK
    return pl.pallas_call(
        dwq_kernel,
        grid=(dim // tile,),
        out_shape=jax.ShapeDtypeStruct((n_heads, dim, BLK), F32),
        in_specs=[pl.BlockSpec((tokens, tile), lambda j: (0, j)), pl.BlockSpec((tokens, wide), lambda j: (0, 0))],
        out_specs=pl.BlockSpec((n_heads, tile, BLK), lambda j: (0, j, 0)),
        compiler_params=pltpu.CompilerParams(vmem_limit_bytes=FULL),
        cost_estimate=pl.CostEstimate(
            flops=2 * tokens * wide * dim, bytes_accessed=2 * tokens * dim + 4 * wide * dim, transcendentals=0
        ),
        name="grad_wq",
    )(x_full, dq)


def split3(a):
    hi = a.astype(BF16)
    rest = a - hi.astype(F32)
    mid = rest.astype(BF16)
    low = (rest - mid.astype(F32)).astype(BF16)
    return hi, mid, low


def kv_kernel(me_ref, mine_ref, other_ref, x_ref, dwk_ref, dwv_ref, rows_ref):
    me = me_ref[0]
    chip = me // 2
    core = lax.rem(me, 2)
    wide = mine_ref.shape[2]
    for p in range(4):
        chunk = jnp.bitwise_xor(chip, p)
        for ref, cls in ((mine_ref, core), (other_ref, 1 - core)):
            rows = pl.ds(pl.multiple_of(chunk * CHUNK + cls * BLK, BLK), BLK)
            for i, piece in enumerate(split3(ref[p])):
                rows_ref[rows, i * wide : (i + 1) * wide] = piece
    res = mm(x_ref[...], rows_ref[...], 0, 0)
    res = res[:, :wide] + res[:, wide : 2 * wide] + res[:, 2 * wide :]
    dwk_ref[...] = res[:, :BLK]
    dwv_ref[...] = res[:, BLK:]


def grad_kv(me, mine, other, x_full, n_dev):
    tokens, dim = x_full.shape
    own = dim // n_dev
    whole = pl.BlockSpec(mine.shape, lambda i, m: (0, 0, 0))
    out = pl.BlockSpec((own, BLK), lambda i, m: (0, 0))
    return pl.pallas_call(
        kv_kernel,
        grid_spec=pltpu.PrefetchScalarGridSpec(
            num_scalar_prefetch=1,
            grid=(1,),
            in_specs=[whole, whole, pl.BlockSpec((tokens, own), lambda i, m: (0, m[0]))],
            out_specs=(out, out),
            scratch_shapes=[pltpu.VMEM((tokens, 3 * mine.shape[2]), BF16)],
        ),
        out_shape=(jax.ShapeDtypeStruct((own, BLK), F32),) * 2,
        compiler_params=pltpu.CompilerParams(vmem_limit_bytes=FULL),
        cost_estimate=pl.CostEstimate(
            flops=2 * tokens * own * 3 * mine.shape[2], bytes_accessed=4 * tokens * own, transcendentals=0
        ),
        name="grad_kv",
    )(me, mine, other, x_full)


def kvdx_kernel(sum_ref, wka_ref, wkb_ref, wva_ref, wvb_ref, pa_ref, pb_ref, oa_ref, ob_ref):
    pieces = split3(sum_ref[0])
    for wk_ref, wv_ref, p_ref, o_ref in (
        (wka_ref, wva_ref, pa_ref, oa_ref),
        (wkb_ref, wvb_ref, pb_ref, ob_ref),
    ):
        w = jnp.concatenate([wk_ref[...], wv_ref[...]], axis=1)
        res = mm(jnp.concatenate(pieces, axis=0), w, 1, 1)
        o_ref[...] = p_ref[...] + (res[:BLK] + res[BLK : 2 * BLK] + res[2 * BLK :])


def kv_dx(total, wk, wv, pa, pb):
    dim, hd = wk.shape
    steps, _, tile = pa.shape
    w_lo = pl.BlockSpec((tile, hd), lambda j: (j, 0))
    w_hi = pl.BlockSpec((tile, hd), lambda j: (j + steps, 0))
    col = pl.BlockSpec((None, BLK, tile), lambda j: (j, 0, 0))
    return pl.pallas_call(
        kvdx_kernel,
        grid=(steps,),
        out_shape=(jax.ShapeDtypeStruct(pa.shape, F32),) * 2,
        in_specs=[pl.BlockSpec((1,) + total.shape[1:], lambda j: (0, 0, 0)), w_lo, w_hi, w_lo, w_hi, col, col],
        out_specs=(col, col),
        compiler_params=pltpu.CompilerParams(vmem_limit_bytes=FULL),
        cost_estimate=pl.CostEstimate(flops=12 * BLK * dim * hd, bytes_accessed=10 * 2**20, transcendentals=0),
        name="kv_dx",
    )(total, wk, wk, wv, wv, pa, pb)


def dx_sum_kernel(steps, a0, a1, a2, b0, b1, b2, out_ref):
    j = pl.program_id(0)

    @pl.when(j < steps)
    def _():
        out_ref[...] = ((a0[...] + a1[...]) + a2[...]).astype(BF16)

    @pl.when(j >= steps)
    def _():
        out_ref[...] = ((b0[...] + b1[...]) + b2[...]).astype(BF16)


def dx_sum(a_terms, b_terms):
    steps, _, tile = a_terms[0].shape
    a_spec = pl.BlockSpec((None, BLK, tile), lambda j: (jnp.minimum(j, steps - 1), 0, 0))
    b_spec = pl.BlockSpec((None, BLK, tile), lambda j: (jnp.maximum(j - steps, 0), 0, 0))
    return pl.pallas_call(
        functools.partial(dx_sum_kernel, steps),
        grid=(2 * steps,),
        out_shape=jax.ShapeDtypeStruct((BLK, 2 * steps * tile), BF16),
        in_specs=[a_spec] * 3 + [b_spec] * 3,
        out_specs=pl.BlockSpec((BLK, tile), lambda j: (0, j)),
        compiler_params=pltpu.CompilerParams(vmem_limit_bytes=FULL),
        cost_estimate=pl.CostEstimate(flops=2**20, bytes_accessed=12 * 2**20, transcendentals=0),
        name="dx_sum",
    )(*a_terms, *b_terms)


def solution(mesh):
    n_dev = mesh.shape["tp"]

    def swap(a, mask):
        return lax.ppermute(a, "tp", [(i, i ^ mask) for i in range(n_dev)])

    def local_grads(x_blk, dy_blk, wq_loc, w_k, w_v, wo_loc):
        n_heads, hd = wq_loc.shape[1:]
        scale = hd ** -0.5
        wide = n_heads * hd
        wq = jnp.transpose(wq_loc, (1, 0, 2))
        wk = w_k[:, 0, :]
        wv = w_v[:, 0, :]
        me = lax.axis_index("tp").astype(jnp.int32).reshape(1)
        (
            xf, dyf, _, _, _, px_a, px_b, py_a, py_b, po_a, po_b, o, dq, kvs, kx0, kx1, ky0, ky1
        ) = front(x_blk, dy_blk, wq, wk, wv, wo_loc, n_dev, scale)
        kd0 = swap(kx0, Y_NBR)
        kd1 = swap(ky1, X_NBR)
        a2 = swap(px_a, X_NBR)
        b2 = swap(py_b, Y_NBR)
        a3 = swap(py_a, Y_NBR)
        b3 = swap(px_b, X_NBR)
        dwo = grad_wo(o, dyf)
        kv_x = (kx0[0], kx0[1], kx1[0], kx1[1])
        kv_y = (ky0[0], ky0[1], ky1[0], ky1[1])
        kv_d = (kd0[0], kd0[1], kd1[0], kd1[1])
        total = jnp.stack([kvs[p] + kv_x[p ^ 1] + kv_y[p ^ 2] + kv_d[p ^ 3] for p in range(4)])
        other = swap(total, SIB)
        dwq = grad_wq(xf, dq)
        base_a, base_b = kv_dx(total, wk, wv, po_a, po_b)
        dwk, dwv = grad_kv(me, total, other, xf, n_dev)
        dx = dx_sum((base_a, a2, a3), (base_b, b2, b3))
        return dx, jnp.transpose(dwq, (1, 0, 2)), dwo, dwk, dwv

    tok_spec = P(("dp", "tp"))
    return jax.shard_map(
        local_grads,
        mesh=mesh,
        in_specs=(tok_spec, tok_spec, P(None, "tp", None), P(), P(), P("tp")),
        out_specs=(tok_spec, P("dp", "tp", None), tok_spec, tok_spec, tok_spec),
        check_vma=False,
    )
```

```python
import functools

import jax
import jax.numpy as jnp
from jax import lax
from jax.experimental import pallas as pl
from jax.experimental.pallas import tpu as pltpu
from jax.sharding import PartitionSpec as P

MESH = pl.DeviceIdType.MESH
F32 = jnp.float32
BF16 = jnp.bfloat16
ANY = pl.BlockSpec(memory_space=pl.ANY)
VM = pl.BlockSpec(memory_space=pltpu.VMEM)
BLK = 128
HALF = 64
FULL = 67043328
CHUNK = 256
X_NBR, Y_NBR, SIB = 2, 4, 1


def mm(a, b, ca, cb):
    return lax.dot_general(a, b, (((ca,), (cb,)), ((), ())), preferred_element_type=F32)


def rows_of(chunk):
    return pl.ds(pl.multiple_of(chunk * CHUNK, CHUNK), CHUNK)


LOG2E = 1.4426950408889634


def attend_chunk(chunk, n_heads, scale, q_ref, do_ref, k_ref, v_ref, put, dkt_ref, dvt_ref):
    for last in range(q_ref.shape[0] // CHUNK):

        @pl.when(chunk == last)
        def _(last=last):
            span = (last + 1) * CHUNK
            rows = pl.ds(last * CHUNK, CHUNK)

            def pair(j, carry):
                keys = k_ref[:span, :]
                vals = v_ref[:span, :]
                row = lax.broadcasted_iota(jnp.int32, (CHUNK, CHUNK), 0)
                col = lax.broadcasted_iota(jnp.int32, (CHUNK, CHUNK), 1)
                got = []
                for h in (2 * j, 2 * j + 1):
                    cols = pl.ds(pl.multiple_of(h * BLK, BLK), BLK)
                    q = q_ref[rows, cols]
                    d_out = do_ref[rows, cols]
                    s = mm(q, keys, 1, 1)
                    s_diag = jnp.where(row >= col, s[:, span - CHUNK :], -jnp.inf)
                    s = s_diag if last == 0 else jnp.concatenate([s[:, : span - CHUNK], s_diag], axis=1)
                    e = jnp.exp2((s - jnp.max(s, axis=1, keepdims=True)) * (scale * LOG2E))
                    p = e * (1.0 / jnp.sum(e, axis=1, keepdims=True))
                    pb = p.astype(BF16)
                    o = mm(pb, vals, 1, 0).astype(BF16)
                    delta = jnp.sum(d_out.astype(F32) * o.astype(F32), axis=1, keepdims=True)
                    ds = (p * (mm(d_out, vals, 1, 1) - delta)).astype(BF16)
                    dq = (mm(ds, keys, 1, 0) * scale).astype(BF16)
                    put(h, o, dq)
                    got.append((q, d_out, pb, ds))
                q2, do2, pb2, ds2 = (jnp.concatenate(both, axis=0) for both in zip(*got))
                dkt_ref[:, :span] += mm(q2, ds2, 0, 0)
                dvt_ref[:, :span] += mm(do2, pb2, 0, 0)
                return carry

            lax.fori_loop(0, n_heads // 2, pair, 0)


def front_kernel(
    n_heads, scale,
    x_ref, dy_ref, wq_ref, wk_ref, wv_ref, wo_ref,
    xf_ref, dyf_ref, wqs_ref, pd_ref, r_ref, pxa_ref, pxb_ref, pya_ref, pyb_ref, poa_ref, pob_ref,
    of_ref, dqf_ref, kvo_ref, kx0_ref, kx1_ref, ky0_ref, ky1_ref,
    xb, yb, wq, wkv, wo, q_ref, do_ref, o_ref, dq_ref, k_ref, v_ref, dk_ref, dv_ref,
    pt, rt, got_q, dkv, got_kv, kvs,
    send_sem, recv_sem, wsem, lsem, osem, gq_send, gq_recv, gkv_send, gkv_recv,
    r_send, r_recv, kn_send, kn_recv, wt_sem, pt_sem, rt_sem, att_sem,
):
    me = lax.axis_index("tp")
    chip = me // 2
    core = lax.rem(me, 2)
    partner = {m: jnp.bitwise_xor(me, m) for m in range(1, 8)}
    barrier = pltpu.get_barrier_semaphore()
    for m in (SIB, X_NBR, Y_NBR):
        pl.semaphore_signal(barrier, inc=1, device_id={"tp": partner[m]}, device_id_type=MESH)
    pl.semaphore_wait(barrier, 3)

    bufs = (xb, yb)
    n_w = wk_ref.shape[0]
    srcs = (x_ref, dy_ref)
    outs = (xf_ref, dyf_ref)
    counts = [0, 0]
    sends = []

    def remote(src, dst, ssem, rsem, mask):
        return pltpu.make_async_remote_copy(
            src_ref=src, dst_ref=dst, send_sem=ssem, recv_sem=rsem,
            device_id={"tp": partner[mask]}, device_id_type=MESH,
        )

    def part(t, block, half):
        return bufs[t].at[block, pl.ds(half * HALF, HALF)]

    def send(t, block, half, mask, own=False):
        src = srcs[t].at[pl.ds(half * HALF, HALF)] if own else part(t, block, half)
        copy = remote(src, part(t, block, half), send_sem.at[t, counts[t]], recv_sem.at[t, block, half], mask)
        counts[t] += 1
        copy.start()
        sends.append(copy)

    def arrive(t, mask, half):
        block = partner[mask]
        here = part(t, block, half)
        remote(here, here, send_sem.at[t, 0], recv_sem.at[t, block, half], SIB).wait_recv()

    for half in range(2):
        send(0, me, half, X_NBR, own=True)
        send(0, me, half, Y_NBR, own=True)
    send(1, me, 0, X_NBR, own=True)
    send(1, me, 1, Y_NBR, own=True)
    loads = [
        pltpu.make_async_copy(x_ref, xb.at[me], lsem.at[0]),
        pltpu.make_async_copy(wq_ref, wq, lsem.at[1]),
        pltpu.make_async_copy(wk_ref, wkv.at[pl.ds(0, n_w)], lsem.at[2]),
        pltpu.make_async_copy(wv_ref, wkv.at[pl.ds(n_w, n_w)], lsem.at[3]),
        pltpu.make_async_copy(dy_ref, yb.at[me], lsem.at[4]),
        pltpu.make_async_copy(wo_ref, wo, lsem.at[5]),
    ]
    for copy in loads:
        copy.start()
    for half in range(2):
        send(0, me, half, SIB, own=True)
    for half in range(2):
        send(1, me, half, SIB, own=True)
    w_copy = remote(wq_ref, wqs_ref, wsem.at[0], wsem.at[1], SIB)
    w_copy.start()
    dk_ref[...] = jnp.zeros_like(dk_ref)
    dv_ref[...] = jnp.zeros_like(dv_ref)

    def chunk_of(p):
        return jnp.bitwise_xor(chip, p)

    def block_rows(p, cls):
        return pl.ds(pl.multiple_of(chunk_of(p) * CHUNK + cls * BLK, BLK), BLK)

    def write_out(t, p):
        chunk = chunk_of(p)
        return [
            pltpu.make_async_copy(
                bufs[t].at[2 * chunk + i],
                outs[t].at[pl.ds(pl.multiple_of((2 * chunk + i) * BLK, BLK), BLK)],
                osem.at[t, p, i],
            )
            for i in range(2)
        ]

    def project(p):
        chunk = chunk_of(p)
        rows = rows_of(chunk)
        x = xb[pl.ds(2 * chunk, 2)].reshape(CHUNK, xb.shape[2])

        def pair(j, carry):
            w = jnp.concatenate([wq[2 * j], wq[2 * j + 1]], axis=1)
            q_ref[rows, pl.ds(pl.multiple_of(j * 2 * BLK, 2 * BLK), 2 * BLK)] = mm(x, w, 1, 0).astype(BF16)
            return carry

        lax.fori_loop(0, n_heads // 2, pair, 0)
        wide_kv = [wkv[g * n_w : (g + 1) * n_w].reshape(n_w * TILE, BLK) for g in range(2)]
        kv = mm(x, jnp.concatenate(wide_kv, axis=1), 1, 0).astype(BF16)
        k_ref[rows, :] = kv[:, :BLK]
        v_ref[rows, :] = kv[:, BLK:]
        for copy in write_out(0, p):
            copy.start()

    def project_out(p):
        chunk = chunk_of(p)
        rows = rows_of(chunk)
        y = yb[pl.ds(2 * chunk, 2)].reshape(CHUNK, yb.shape[2])

        def pair(j, carry):
            w = wo[pl.ds(2 * j, 2)].reshape(2 * BLK, wo.shape[2])
            do_ref[rows, pl.ds(pl.multiple_of(j * 2 * BLK, 2 * BLK), 2 * BLK)] = mm(y, w, 1, 1).astype(BF16)
            return carry

        lax.fori_loop(0, n_heads // 2, pair, 0)
        for copy in write_out(1, p):
            copy.start()

    def both(t, mask):
        arrive(t, mask, 0)
        arrive(t, mask, 1)

    def attend_rows(p):
        chunk = chunk_of(p)
        rows = rows_of(chunk)

        def put(h, o, dq):
            cols = pl.ds(pl.multiple_of(h * BLK, BLK), BLK)
            o_ref[rows, cols] = o
            dq_ref[rows, cols] = dq

        attend_chunk(chunk, n_heads, scale, q_ref, do_ref, k_ref, v_ref, put, dk_ref, dv_ref)

    def att_out(p):
        rows = rows_of(chunk_of(p))
        return (
            pltpu.make_async_copy(o_ref.at[rows], of_ref.at[rows], att_sem.at[p, 0]),
            pltpu.make_async_copy(dq_ref.at[rows], dqf_ref.at[rows], att_sem.at[p, 1]),
        )

    def give_q(p):
        return remote(dq_ref.at[block_rows(p, 1 - core)], got_q.at[p], gq_send.at[p], gq_recv.at[p], SIB)

    def give_kv(p):
        return remote(dkv.at[block_rows(p, 1 - core)], got_kv.at[p], gkv_send.at[p], gkv_recv.at[p], SIB)

    tile = wkv.shape[1]
    steps = pd_ref.shape[1]

    def w_load(side, i):
        col = pl.multiple_of((side * steps + i) * tile, tile)
        slot = lax.rem(2 * i + side, W_SLOTS)
        return pltpu.make_async_copy(wqs_ref.at[:, pl.ds(col, tile), :], wkv.at[pl.ds(slot * n_heads, n_heads)], wt_sem.at[slot])

    def w_ahead(side, i):
        t = 2 * i + side + W_SLOTS - 1

        @pl.when(t < 2 * steps)
        def _():
            w_load(lax.rem(t, 2), t // 2).start()

    def w_first():
        for t in range(W_SLOTS - 1):
            w_load(t % 2, t // 2).start()

    def product(groups, side, i):
        col = pl.multiple_of((side * steps + i) * tile, tile)
        lhs = jnp.concatenate(
            [
                jnp.concatenate([dq_ref[block_rows(p, core), :] for p in groups], axis=0),
                jnp.concatenate([got_q[p] for p in groups], axis=0),
            ],
            axis=1,
        )
        rhs = jnp.concatenate(
            [wq[h, pl.ds(col, tile), :] for h in range(n_heads)] + [wkv[lax.rem(2 * i + side, W_SLOTS) * n_heads + h] for h in range(n_heads)], axis=1
        )
        return mm(lhs, rhs, 1, 1)

    for copy in loads[:4]:
        copy.wait()
    both(0, SIB)
    project(0)
    for copy in loads[4:]:
        copy.wait()
    both(1, SIB)
    project_out(0)
    arrive(0, X_NBR, 0)
    send(0, partner[X_NBR], 0, Y_NBR)
    arrive(0, Y_NBR, 1)
    send(0, partner[Y_NBR], 1, X_NBR)
    send(0, partner[X_NBR], 0, SIB)
    send(0, partner[Y_NBR], 1, SIB)
    arrive(0, X_NBR, 1)
    send(0, partner[X_NBR], 1, SIB)
    arrive(0, Y_NBR, 0)
    send(0, partner[Y_NBR], 0, SIB)
    both(0, X_NBR ^ SIB)
    project(1)
    both(0, Y_NBR ^ SIB)
    project(2)
    arrive(1, X_NBR, 0)
    send(1, partner[X_NBR], 0, Y_NBR)
    arrive(1, Y_NBR, 1)
    send(1, partner[Y_NBR], 1, X_NBR)
    send(1, me, 1, X_NBR, own=True)
    send(1, me, 0, Y_NBR, own=True)
    send(1, partner[X_NBR], 0, SIB)
    send(1, partner[Y_NBR], 1, SIB)
    diag = X_NBR ^ Y_NBR
    for t in range(2):
        for half in range(2):
            arrive(t, diag, half)
            send(t, partner[diag], half, SIB)
        both(t, diag ^ SIB)
        if t == 0:
            project(3)
        else:
            project_out(3)

    def pd_write(side, i):
        return pltpu.make_async_copy(pt.at[side, pl.ds(0, BLK)], pd_ref.at[side, i], pt_sem.at[side, 0])

    def round1(side, i):
        return pltpu.make_async_remote_copy(
            src_ref=pd_ref.at[side, i], dst_ref=r_ref.at[side, i],
            send_sem=r_send.at[side, i], recv_sem=r_recv.at[side, i],
            device_id={"tp": jnp.bitwise_xor(me, X_NBR * (1 + side))}, device_id_type=MESH,
        )

    def pd_step(i, carry):
        for side in range(2):
            w_load(side, i).wait()
            w_ahead(side, i)
            res = product((3,), side, i)

            @pl.when(i > 0)
            def _(side=side):
                pd_write(side, i - 1).wait()
                round1(side, i - 1).start()

            pt[side, :BLK] = res
            pd_write(side, i).start()

        return carry

    def late(i):
        block, half = ((partner[X_NBR], 1), (partner[Y_NBR], 0))[i]
        here = part(1, block, half)
        return remote(here, here, send_sem.at[1, counts[1] + i], recv_sem.at[1, block, half], SIB)

    def rows_step(i, carry):
        p = 3 - i
        attend_rows(p)
        give_q(p).start()
        for copy in att_out(p):
            copy.start()

        @pl.when(i == 0)
        def _():
            w_copy.wait()
            w_first()
            give_q(3).wait_recv()
            lax.fori_loop(0, steps, pd_step, 0)
            for side in range(2):
                pd_write(side, steps - 1).wait()
                round1(side, steps - 1).start()
            w_first()
            arrive(1, X_NBR, 1)
            late(0).start()
            arrive(1, Y_NBR, 0)
            late(1).start()
            both(1, X_NBR ^ SIB)
            project_out(1)
            both(1, Y_NBR ^ SIB)
            project_out(2)

        return carry

    lax.fori_loop(0, 4, rows_step, 0)
    dkv[:, :BLK] = (dk_ref[...].T * scale).astype(BF16)
    dkv[:, BLK:] = dv_ref[...].T.astype(BF16)
    for p in range(3):
        give_q(p).wait_recv()
    for p in range(4):
        give_kv(p).start()

    def r_load(side, i):
        slot = lax.rem(2 * i + side, R_SLOTS)
        return pltpu.make_async_copy(r_ref.at[side, i], rt.at[slot], rt_sem.at[slot])

    def r_ahead(side, i):
        t = 2 * i + side + R_SLOTS - 1

        @pl.when(t < 2 * steps)
        def _():
            round1(lax.rem(t, 2), t // 2).wait_recv()
            r_load(lax.rem(t, 2), t // 2).start()

    groups = (1, 2, 0)
    targets = ((pxa_ref, pya_ref, poa_ref), (pxb_ref, pyb_ref, pob_ref))

    def p_writes(side, i):
        return [
            pltpu.make_async_copy(pt.at[side, pl.ds(g * BLK, BLK)], targets[side][g].at[i], pt_sem.at[side, g])
            for g in range(3)
        ]

    def p_step(i, carry):
        for side in range(2):
            w_load(side, i).wait()
            w_ahead(side, i)
            r_ahead(side, i)
            res = product(groups, side, i)

            @pl.when(i > 0)
            def _(side=side):
                for copy in p_writes(side, i - 1):
                    copy.wait()

            r_load(side, i).wait()
            add = 1 - side
            for g in range(3):
                rows = res[g * BLK : (g + 1) * BLK]
                pt[side, g * BLK : (g + 1) * BLK] = rows + rt[lax.rem(2 * i + side, R_SLOTS)] if g == add else rows
            for copy in p_writes(side, i):
                copy.start()

        return carry

    for t in range(R_SLOTS - 1):
        round1(t % 2, t // 2).wait_recv()
        r_load(t % 2, t // 2).start()
    for p in range(4):
        give_kv(p).wait_recv()
        kvs[p] = dkv[block_rows(p, core), :].astype(F32) + got_kv[p].astype(F32)
    p_step(0, 0)
    near = [
        remote(kvs.at[pl.ds(2 * i, 2)], dst, kn_send.at[n, i], kn_recv.at[n, i], mask)
        for n, (mask, dsts) in enumerate(((X_NBR, (kx0_ref, kx1_ref)), (Y_NBR, (ky0_ref, ky1_ref))))
        for i, dst in enumerate(dsts)
    ]
    for copy in near:
        copy.start()
    kv_out = pltpu.make_async_copy(kvs, kvo_ref, lsem.at[0])
    kv_out.start()
    lax.fori_loop(1, steps, p_step, 0)
    for side in range(2):
        for copy in p_writes(side, steps - 1):
            copy.wait()
    for copy in sends:
        copy.wait_send()
    for i in range(2):
        late(i).wait_send()
    for p in range(4):
        give_q(p).wait_send()
        give_kv(p).wait_send()
        for copy in att_out(p):
            copy.wait()
    for side in range(2):
        for i in range(steps):
            round1(side, i).wait_send()
    for copy in near:
        copy.wait()
    kv_out.wait()
    for t in range(2):
        for p in range(4):
            for copy in write_out(t, p):
                copy.wait()


TILE = 512
W_SLOTS = 4
R_SLOTS = 4


def front(x_blk, dy_blk, wq, wk, wv, wo, n_dev, scale):
    n_heads, dim, hd = wq.shape
    tokens = x_blk.shape[0] * n_dev
    wide = n_heads * hd
    steps = dim // 2 // TILE
    sds = jax.ShapeDtypeStruct
    sem = pltpu.SemaphoreType.DMA
    piece = sds((steps, BLK, TILE), F32)
    return pl.pallas_call(
        functools.partial(front_kernel, n_heads, scale),
        out_shape=(
            sds((tokens, dim), BF16), sds((tokens, dim), BF16), sds(wq.shape, BF16),
            sds((2, steps, BLK, TILE), F32), sds((2, steps, BLK, TILE), F32),
            piece, piece, piece, piece, piece, piece,
            sds((tokens, wide), BF16), sds((tokens, wide), BF16), sds((4, BLK, 2 * hd), F32),
        )
        + (sds((2, BLK, 2 * hd), F32),) * 4,
        in_specs=[ANY] * 6,
        out_specs=(ANY,) * 18,
        scratch_shapes=[
            pltpu.VMEM((n_dev, BLK, dim), BF16),
            pltpu.VMEM((n_dev, BLK, dim), BF16),
            pltpu.VMEM(wq.shape, BF16),
            pltpu.VMEM((max(2 * dim // TILE, W_SLOTS * n_heads), TILE, hd), BF16),
            pltpu.VMEM(wo.shape, BF16),
            pltpu.VMEM((tokens, wide), BF16),
            pltpu.VMEM((tokens, wide), BF16),
            pltpu.VMEM((tokens, wide), BF16),
            pltpu.VMEM((tokens, wide), BF16),
            pltpu.VMEM((tokens, hd), BF16),
            pltpu.VMEM((tokens, hd), BF16),
            pltpu.VMEM((hd, tokens), F32),
            pltpu.VMEM((hd, tokens), F32),
            pltpu.VMEM((2, 3 * BLK, TILE), F32),
            pltpu.VMEM((R_SLOTS, BLK, TILE), F32),
            pltpu.VMEM((4, BLK, wide), BF16),
            pltpu.VMEM((tokens, 2 * hd), BF16),
            pltpu.VMEM((4, BLK, 2 * hd), BF16),
            pltpu.VMEM((4, BLK, 2 * hd), F32),
            sem((2, 14)), sem((2, n_dev, 2)), sem((2,)), sem((6,)), sem((2, 4, 2)),
            sem((4,)), sem((4,)), sem((4,)), sem((4,)),
            sem((2, steps)), sem((2, steps)), sem((2, 2)), sem((2, 2)),
            sem((W_SLOTS,)), sem((2, 3)), sem((R_SLOTS,)), sem((4, 2)),
        ],
        compiler_params=pltpu.CompilerParams(collective_id=0, has_side_effects=True, vmem_limit_bytes=FULL),
        name="front",
    )(x_blk, dy_blk, wq, wk.reshape(-1, TILE, hd), wv.reshape(-1, TILE, hd), wo)


def dwo_kernel(o_ref, dy_ref, out_ref, o_t):
    @pl.when(pl.program_id(0) == 0)
    def _():
        o_t[...] = o_ref[...].T

    res = mm(o_t[...], dy_ref[...], 1, 0)
    for h in range(out_ref.shape[0]):
        out_ref[h] = res[h * BLK : (h + 1) * BLK]


def grad_wo(o, dy_full):
    tokens, wide = o.shape
    dim = dy_full.shape[1]
    tile = 512
    n_heads = wide // BLK
    return pl.pallas_call(
        dwo_kernel,
        grid=(dim // tile,),
        out_shape=jax.ShapeDtypeStruct((n_heads, BLK, dim), F32),
        in_specs=[pl.BlockSpec((tokens, wide), lambda j: (0, 0)), pl.BlockSpec((tokens, tile), lambda j: (0, j))],
        out_specs=pl.BlockSpec((n_heads, BLK, tile), lambda j: (0, 0, j)),
        scratch_shapes=[pltpu.VMEM((wide, tokens), BF16)],
        compiler_params=pltpu.CompilerParams(vmem_limit_bytes=FULL),
        cost_estimate=pl.CostEstimate(
            flops=2 * tokens * wide * dim, bytes_accessed=2 * tokens * dim + 4 * wide * dim, transcendentals=0
        ),
        name="grad_wo",
    )(o, dy_full)


def dwq_kernel(x_ref, dq_ref, out_ref):
    res = mm(x_ref[...], dq_ref[...], 0, 0)
    for h in range(out_ref.shape[0]):
        out_ref[h] = res[:, h * BLK : (h + 1) * BLK]


def grad_wq(x_full, dq):
    tokens, wide = dq.shape
    dim = x_full.shape[1]
    tile = 512
    n_heads = wide // BLK
    return pl.pallas_call(
        dwq_kernel,
        grid=(dim // tile,),
        out_shape=jax.ShapeDtypeStruct((n_heads, dim, BLK), F32),
        in_specs=[pl.BlockSpec((tokens, tile), lambda j: (0, j)), pl.BlockSpec((tokens, wide), lambda j: (0, 0))],
        out_specs=pl.BlockSpec((n_heads, tile, BLK), lambda j: (0, j, 0)),
        compiler_params=pltpu.CompilerParams(vmem_limit_bytes=FULL),
        cost_estimate=pl.CostEstimate(
            flops=2 * tokens * wide * dim, bytes_accessed=2 * tokens * dim + 4 * wide * dim, transcendentals=0
        ),
        name="grad_wq",
    )(x_full, dq)


def split3(a):
    hi = a.astype(BF16)
    rest = a - hi.astype(F32)
    mid = rest.astype(BF16)
    low = (rest - mid.astype(F32)).astype(BF16)
    return hi, mid, low


def kv_kernel(me_ref, mine_ref, other_ref, x_ref, dwk_ref, dwv_ref, rows_ref):
    me = me_ref[0]
    chip = me // 2
    core = lax.rem(me, 2)
    wide = mine_ref.shape[2]
    for p in range(4):
        chunk = jnp.bitwise_xor(chip, p)
        for ref, cls in ((mine_ref, core), (other_ref, 1 - core)):
            rows = pl.ds(pl.multiple_of(chunk * CHUNK + cls * BLK, BLK), BLK)
            for i, piece in enumerate(split3(ref[p])):
                rows_ref[rows, i * wide : (i + 1) * wide] = piece
    res = mm(x_ref[...], rows_ref[...], 0, 0)
    res = res[:, :wide] + res[:, wide : 2 * wide] + res[:, 2 * wide :]
    dwk_ref[...] = res[:, :BLK]
    dwv_ref[...] = res[:, BLK:]


def grad_kv(me, mine, other, x_full, n_dev):
    tokens, dim = x_full.shape
    own = dim // n_dev
    whole = pl.BlockSpec(mine.shape, lambda i, m: (0, 0, 0))
    out = pl.BlockSpec((own, BLK), lambda i, m: (0, 0))
    return pl.pallas_call(
        kv_kernel,
        grid_spec=pltpu.PrefetchScalarGridSpec(
            num_scalar_prefetch=1,
            grid=(1,),
            in_specs=[whole, whole, pl.BlockSpec((tokens, own), lambda i, m: (0, m[0]))],
            out_specs=(out, out),
            scratch_shapes=[pltpu.VMEM((tokens, 3 * mine.shape[2]), BF16)],
        ),
        out_shape=(jax.ShapeDtypeStruct((own, BLK), F32),) * 2,
        compiler_params=pltpu.CompilerParams(vmem_limit_bytes=FULL),
        cost_estimate=pl.CostEstimate(
            flops=2 * tokens * own * 3 * mine.shape[2], bytes_accessed=4 * tokens * own, transcendentals=0
        ),
        name="grad_kv",
    )(me, mine, other, x_full)


def kvdx_kernel(sum_ref, wka_ref, wkb_ref, wva_ref, wvb_ref, pa_ref, pb_ref, ra_ref, rb_ref, oa_ref, ob_ref):
    pieces = split3(sum_ref[0])
    for wk_ref, wv_ref, p_ref, r_ref, o_ref in (
        (wka_ref, wva_ref, pa_ref, ra_ref, oa_ref),
        (wkb_ref, wvb_ref, pb_ref, rb_ref, ob_ref),
    ):
        w = jnp.concatenate([wk_ref[...], wv_ref[...]], axis=1)
        res = mm(jnp.concatenate(pieces, axis=0), w, 1, 1)
        o_ref[...] = (p_ref[...] + r_ref[...]) + (res[:BLK] + res[BLK : 2 * BLK] + res[2 * BLK :])


def kv_dx(total, wk, wv, pa, pb, ra, rb):
    dim, hd = wk.shape
    steps, _, tile = pa.shape
    w_lo = pl.BlockSpec((tile, hd), lambda j: (j, 0))
    w_hi = pl.BlockSpec((tile, hd), lambda j: (j + steps, 0))
    col = pl.BlockSpec((None, BLK, tile), lambda j: (j, 0, 0))
    return pl.pallas_call(
        kvdx_kernel,
        grid=(steps,),
        out_shape=(jax.ShapeDtypeStruct(pa.shape, F32),) * 2,
        in_specs=[pl.BlockSpec((1,) + total.shape[1:], lambda j: (0, 0, 0)), w_lo, w_hi, w_lo, w_hi, col, col, col, col],
        out_specs=(col, col),
        compiler_params=pltpu.CompilerParams(vmem_limit_bytes=FULL),
        cost_estimate=pl.CostEstimate(flops=12 * BLK * dim * hd, bytes_accessed=10 * 2**20, transcendentals=0),
        name="kv_dx",
    )(total, wk, wk, wv, wv, pa, pb, ra, rb)


GROUP = 3


def dx_sum_kernel(groups, a0, a1, b0, b1, out_ref):
    j = pl.program_id(0)
    tile = a0.shape[2]

    def add(x, y):
        for g in range(GROUP):
            out_ref[:, g * tile : (g + 1) * tile] = (x[g] + y[g]).astype(BF16)

    pl.when(j < groups)(lambda: add(a0, a1))
    pl.when(j >= groups)(lambda: add(b0, b1))


def dx_sum(a_terms, b_terms):
    steps, _, tile = a_terms[0].shape
    groups = steps // GROUP
    a_spec = pl.BlockSpec((GROUP, BLK, tile), lambda j: (jnp.minimum(j, groups - 1), 0, 0))
    b_spec = pl.BlockSpec((GROUP, BLK, tile), lambda j: (jnp.maximum(j - groups, 0), 0, 0))
    return pl.pallas_call(
        functools.partial(dx_sum_kernel, groups),
        grid=(2 * groups,),
        out_shape=jax.ShapeDtypeStruct((BLK, 2 * steps * tile), BF16),
        in_specs=[a_spec] * 2 + [b_spec] * 2,
        out_specs=pl.BlockSpec((BLK, GROUP * tile), lambda j: (0, j)),
        compiler_params=pltpu.CompilerParams(vmem_limit_bytes=FULL),
        cost_estimate=pl.CostEstimate(flops=2**20, bytes_accessed=8 * 2**20, transcendentals=0),
        name="dx_sum",
    )(*a_terms, *b_terms)


def solution(mesh):
    n_dev = mesh.shape["tp"]

    def swap(a, mask):
        return lax.ppermute(a, "tp", [(i, i ^ mask) for i in range(n_dev)])

    def local_grads(x_blk, dy_blk, wq_loc, w_k, w_v, wo_loc):
        n_heads, hd = wq_loc.shape[1:]
        scale = hd ** -0.5
        wide = n_heads * hd
        wq = jnp.transpose(wq_loc, (1, 0, 2))
        wk = w_k[:, 0, :]
        wv = w_v[:, 0, :]
        me = lax.axis_index("tp").astype(jnp.int32).reshape(1)
        (
            xf, dyf, _, _, _, px_a, px_b, py_a, py_b, po_a, po_b, o, dq, kvs, kx0, kx1, ky0, ky1
        ) = front(x_blk, dy_blk, wq, wk, wv, wo_loc, n_dev, scale)
        kd0 = swap(kx0, Y_NBR)
        kd1 = swap(ky1, X_NBR)
        a2 = swap(px_a, X_NBR)
        b2 = swap(py_b, Y_NBR)
        a3 = swap(py_a, Y_NBR)
        b3 = swap(px_b, X_NBR)
        dwo = grad_wo(o, dyf)
        kv_x = (kx0[0], kx0[1], kx1[0], kx1[1])
        kv_y = (ky0[0], ky0[1], ky1[0], ky1[1])
        kv_d = (kd0[0], kd0[1], kd1[0], kd1[1])
        total = jnp.stack([kvs[p] + kv_x[p ^ 1] + kv_y[p ^ 2] + kv_d[p ^ 3] for p in range(4)])
        other = swap(total, SIB)
        dwq = grad_wq(xf, dq)
        base_a, base_b = kv_dx(total, wk, wv, po_a, po_b, a2, b2)
        dwk, dwv = grad_kv(me, total, other, xf, n_dev)
        dx = dx_sum((base_a, a3), (base_b, b3))
        return dx, jnp.transpose(dwq, (1, 0, 2)), dwo, dwk, dwv

    tok_spec = P(("dp", "tp"))
    return jax.shard_map(
        local_grads,
        mesh=mesh,
        in_specs=(tok_spec, tok_spec, P(None, "tp", None), P(), P(), P("tp")),
        out_specs=(tok_spec, P("dp", "tp", None), tok_spec, tok_spec, tok_spec),
        check_vma=False,
    )
```

```python
import functools

import jax
import jax.numpy as jnp
from jax import lax
from jax.experimental import pallas as pl
from jax.experimental.pallas import tpu as pltpu
from jax.sharding import PartitionSpec as P

MESH = pl.DeviceIdType.MESH
F32 = jnp.float32
BF16 = jnp.bfloat16
ANY = pl.BlockSpec(memory_space=pl.ANY)
VM = pl.BlockSpec(memory_space=pltpu.VMEM)
BLK = 128
HALF = 64
FULL = 67043328
CHUNK = 256
X_NBR, Y_NBR, SIB = 2, 4, 1


def mm(a, b, ca, cb):
    return lax.dot_general(a, b, (((ca,), (cb,)), ((), ())), preferred_element_type=F32)


def rows_of(chunk):
    return pl.ds(pl.multiple_of(chunk * CHUNK, CHUNK), CHUNK)


LOG2E = 1.4426950408889634


def attend_chunk(chunk, n_heads, scale, q_ref, do_ref, k_ref, v_ref, put, dkt_ref, dvt_ref):
    for last in range(q_ref.shape[0] // CHUNK):

        @pl.when(chunk == last)
        def _(last=last):
            span = (last + 1) * CHUNK
            rows = pl.ds(last * CHUNK, CHUNK)

            def pair(j, carry):
                keys = k_ref[:span, :]
                vals = v_ref[:span, :]
                row = lax.broadcasted_iota(jnp.int32, (CHUNK, CHUNK), 0)
                col = lax.broadcasted_iota(jnp.int32, (CHUNK, CHUNK), 1)
                got = []
                for h in (2 * j, 2 * j + 1):
                    cols = pl.ds(pl.multiple_of(h * BLK, BLK), BLK)
                    q = q_ref[rows, cols]
                    d_out = do_ref[rows, cols]
                    s = mm(q, keys, 1, 1)
                    s_diag = jnp.where(row >= col, s[:, span - CHUNK :], -jnp.inf)
                    s = s_diag if last == 0 else jnp.concatenate([s[:, : span - CHUNK], s_diag], axis=1)
                    e = jnp.exp2((s - jnp.max(s, axis=1, keepdims=True)) * (scale * LOG2E))
                    p = e * (1.0 / jnp.sum(e, axis=1, keepdims=True))
                    pb = p.astype(BF16)
                    o = mm(pb, vals, 1, 0).astype(BF16)
                    delta = jnp.sum(d_out.astype(F32) * o.astype(F32), axis=1, keepdims=True)
                    ds = (p * (mm(d_out, vals, 1, 1) - delta)).astype(BF16)
                    dq = (mm(ds, keys, 1, 0) * scale).astype(BF16)
                    put(h, o, dq)
                    got.append((q, d_out, pb, ds))
                q2, do2, pb2, ds2 = (jnp.concatenate(both, axis=0) for both in zip(*got))
                dkt_ref[:, :span] += mm(q2, ds2, 0, 0)
                dvt_ref[:, :span] += mm(do2, pb2, 0, 0)
                return carry

            lax.fori_loop(0, n_heads // 2, pair, 0)


def front_kernel(
    n_heads, scale,
    x_ref, dy_ref, wq_ref, wk_ref, wv_ref, wo_ref,
    xf_ref, dyf_ref, wqs_ref, pd_ref, r_ref, pxa_ref, pxb_ref, pya_ref, pyb_ref, poa_ref, pob_ref,
    of_ref, dqf_ref, kvo_ref, kx0_ref, kx1_ref, ky0_ref, ky1_ref,
    xb, yb, wq, wkv, wo, q_ref, do_ref, o_ref, dq_ref, k_ref, v_ref, dk_ref, dv_ref,
    pt, rt, got_q, dkv, got_kv, kvs,
    send_sem, recv_sem, wsem, lsem, osem, gq_send, gq_recv, gkv_send, gkv_recv,
    r_send, r_recv, kn_send, kn_recv, wt_sem, pt_sem, rt_sem, att_sem,
):
    me = lax.axis_index("tp")
    chip = me // 2
    core = lax.rem(me, 2)
    partner = {m: jnp.bitwise_xor(me, m) for m in range(1, 8)}
    barrier = pltpu.get_barrier_semaphore()
    for m in (SIB, X_NBR, Y_NBR):
        pl.semaphore_signal(barrier, inc=1, device_id={"tp": partner[m]}, device_id_type=MESH)
    pl.semaphore_wait(barrier, 3)

    bufs = (xb, yb)
    n_w = wk_ref.shape[0]
    srcs = (x_ref, dy_ref)
    outs = (xf_ref, dyf_ref)
    counts = [0, 0]
    sends = []

    def remote(src, dst, ssem, rsem, mask):
        return pltpu.make_async_remote_copy(
            src_ref=src, dst_ref=dst, send_sem=ssem, recv_sem=rsem,
            device_id={"tp": partner[mask]}, device_id_type=MESH,
        )

    def part(t, block, half):
        return bufs[t].at[block, pl.ds(half * HALF, HALF)]

    def send(t, block, half, mask, own=False):
        src = srcs[t].at[pl.ds(half * HALF, HALF)] if own else part(t, block, half)
        copy = remote(src, part(t, block, half), send_sem.at[t, counts[t]], recv_sem.at[t, block, half], mask)
        counts[t] += 1
        copy.start()
        sends.append(copy)

    def arrive(t, mask, half):
        block = partner[mask]
        here = part(t, block, half)
        remote(here, here, send_sem.at[t, 0], recv_sem.at[t, block, half], SIB).wait_recv()

    for half in range(2):
        send(0, me, half, X_NBR, own=True)
        send(0, me, half, Y_NBR, own=True)
    send(1, me, 0, X_NBR, own=True)
    send(1, me, 1, Y_NBR, own=True)
    loads = [
        pltpu.make_async_copy(x_ref, xb.at[me], lsem.at[0]),
        pltpu.make_async_copy(wq_ref, wq, lsem.at[1]),
        pltpu.make_async_copy(wk_ref, wkv.at[pl.ds(0, n_w)], lsem.at[2]),
        pltpu.make_async_copy(wv_ref, wkv.at[pl.ds(n_w, n_w)], lsem.at[3]),
        pltpu.make_async_copy(dy_ref, yb.at[me], lsem.at[4]),
        pltpu.make_async_copy(wo_ref, wo, lsem.at[5]),
    ]
    for copy in loads:
        copy.start()
    for half in range(2):
        send(0, me, half, SIB, own=True)
    for half in range(2):
        send(1, me, half, SIB, own=True)
    w_copy = remote(wq_ref, wqs_ref, wsem.at[0], wsem.at[1], SIB)
    w_copy.start()
    dk_ref[...] = jnp.zeros_like(dk_ref)
    dv_ref[...] = jnp.zeros_like(dv_ref)

    def chunk_of(p):
        return jnp.bitwise_xor(chip, p)

    def block_rows(p, cls):
        return pl.ds(pl.multiple_of(chunk_of(p) * CHUNK + cls * BLK, BLK), BLK)

    def write_out(t, p):
        chunk = chunk_of(p)
        return [
            pltpu.make_async_copy(
                bufs[t].at[2 * chunk + i],
                outs[t].at[pl.ds(pl.multiple_of((2 * chunk + i) * BLK, BLK), BLK)],
                osem.at[t, p, i],
            )
            for i in range(2)
        ]

    def project(p):
        chunk = chunk_of(p)
        rows = rows_of(chunk)
        x = xb[pl.ds(2 * chunk, 2)].reshape(CHUNK, xb.shape[2])

        def pair(j, carry):
            w = jnp.concatenate([wq[2 * j], wq[2 * j + 1]], axis=1)
            q_ref[rows, pl.ds(pl.multiple_of(j * 2 * BLK, 2 * BLK), 2 * BLK)] = mm(x, w, 1, 0).astype(BF16)
            return carry

        lax.fori_loop(0, n_heads // 2, pair, 0)
        wide_kv = [wkv[g * n_w : (g + 1) * n_w].reshape(n_w * TILE, BLK) for g in range(2)]
        kv = mm(x, jnp.concatenate(wide_kv, axis=1), 1, 0).astype(BF16)
        k_ref[rows, :] = kv[:, :BLK]
        v_ref[rows, :] = kv[:, BLK:]
        for copy in write_out(0, p):
            copy.start()

    def project_out(p):
        chunk = chunk_of(p)
        rows = rows_of(chunk)
        y = yb[pl.ds(2 * chunk, 2)].reshape(CHUNK, yb.shape[2])

        def pair(j, carry):
            w = wo[pl.ds(2 * j, 2)].reshape(2 * BLK, wo.shape[2])
            do_ref[rows, pl.ds(pl.multiple_of(j * 2 * BLK, 2 * BLK), 2 * BLK)] = mm(y, w, 1, 1).astype(BF16)
            return carry

        lax.fori_loop(0, n_heads // 2, pair, 0)
        for copy in write_out(1, p):
            copy.start()

    def both(t, mask):
        arrive(t, mask, 0)
        arrive(t, mask, 1)

    def attend_rows(p):
        chunk = chunk_of(p)
        rows = rows_of(chunk)

        def put(h, o, dq):
            cols = pl.ds(pl.multiple_of(h * BLK, BLK), BLK)
            o_ref[rows, cols] = o
            dq_ref[rows, cols] = dq

        attend_chunk(chunk, n_heads, scale, q_ref, do_ref, k_ref, v_ref, put, dk_ref, dv_ref)

    def att_out(p):
        rows = rows_of(chunk_of(p))
        return (
            pltpu.make_async_copy(o_ref.at[rows], of_ref.at[rows], att_sem.at[p, 0]),
            pltpu.make_async_copy(dq_ref.at[rows], dqf_ref.at[rows], att_sem.at[p, 1]),
        )

    def give_q(p):
        return remote(dq_ref.at[block_rows(p, 1 - core)], got_q.at[p], gq_send.at[p], gq_recv.at[p], SIB)

    def give_kv(p):
        return remote(dkv.at[block_rows(p, 1 - core)], got_kv.at[p], gkv_send.at[p], gkv_recv.at[p], SIB)

    tile = wkv.shape[1]
    steps = pd_ref.shape[1]

    def w_load(side, i):
        col = pl.multiple_of((side * steps + i) * tile, tile)
        slot = lax.rem(2 * i + side, W_SLOTS)
        return pltpu.make_async_copy(wqs_ref.at[:, pl.ds(col, tile), :], wkv.at[pl.ds(slot * n_heads, n_heads)], wt_sem.at[slot])

    def w_ahead(side, i):
        t = 2 * i + side + W_SLOTS - 1

        @pl.when(t < 2 * steps)
        def _():
            w_load(lax.rem(t, 2), t // 2).start()

    def w_first():
        for t in range(W_SLOTS - 1):
            w_load(t % 2, t // 2).start()

    def product(groups, side, i):
        col = pl.multiple_of((side * steps + i) * tile, tile)
        lhs = jnp.concatenate(
            [
                jnp.concatenate([dq_ref[block_rows(p, core), :] for p in groups], axis=0),
                jnp.concatenate([got_q[p] for p in groups], axis=0),
            ],
            axis=1,
        )
        rhs = jnp.concatenate(
            [wq[h, pl.ds(col, tile), :] for h in range(n_heads)] + [wkv[lax.rem(2 * i + side, W_SLOTS) * n_heads + h] for h in range(n_heads)], axis=1
        )
        return mm(lhs, rhs, 1, 1)

    for copy in loads[:4]:
        copy.wait()
    both(0, SIB)
    project(0)
    for copy in loads[4:]:
        copy.wait()
    both(1, SIB)
    project_out(0)
    arrive(0, X_NBR, 0)
    send(0, partner[X_NBR], 0, Y_NBR)
    arrive(0, Y_NBR, 1)
    send(0, partner[Y_NBR], 1, X_NBR)
    send(0, partner[X_NBR], 0, SIB)
    send(0, partner[Y_NBR], 1, SIB)
    arrive(0, X_NBR, 1)
    send(0, partner[X_NBR], 1, SIB)
    arrive(0, Y_NBR, 0)
    send(0, partner[Y_NBR], 0, SIB)
    both(0, X_NBR ^ SIB)
    project(1)
    both(0, Y_NBR ^ SIB)
    project(2)
    arrive(1, X_NBR, 0)
    send(1, partner[X_NBR], 0, Y_NBR)
    arrive(1, Y_NBR, 1)
    send(1, partner[Y_NBR], 1, X_NBR)
    send(1, me, 1, X_NBR, own=True)
    send(1, me, 0, Y_NBR, own=True)
    send(1, partner[X_NBR], 0, SIB)
    send(1, partner[Y_NBR], 1, SIB)
    diag = X_NBR ^ Y_NBR
    for t in range(2):
        for half in range(2):
            arrive(t, diag, half)
            send(t, partner[diag], half, SIB)
        both(t, diag ^ SIB)
        if t == 0:
            project(3)
        else:
            project_out(3)

    def pd_write(side, i):
        return pltpu.make_async_copy(pt.at[side, pl.ds(0, BLK)], pd_ref.at[side, i], pt_sem.at[side, 0])

    def round1(side, i):
        return pltpu.make_async_remote_copy(
            src_ref=pd_ref.at[side, i], dst_ref=r_ref.at[side, i],
            send_sem=r_send.at[side, i], recv_sem=r_recv.at[side, i],
            device_id={"tp": jnp.bitwise_xor(me, X_NBR * (1 + side))}, device_id_type=MESH,
        )

    def pd_step(i, carry):
        for side in range(2):
            w_load(side, i).wait()
            w_ahead(side, i)
            res = product((3,), side, i)

            @pl.when(i > 0)
            def _(side=side):
                pd_write(side, i - 1).wait()
                round1(side, i - 1).start()

            pt[side, :BLK] = res
            pd_write(side, i).start()

        return carry

    def late(i):
        block, half = ((partner[X_NBR], 1), (partner[Y_NBR], 0))[i]
        here = part(1, block, half)
        return remote(here, here, send_sem.at[1, counts[1] + i], recv_sem.at[1, block, half], SIB)

    def rows_step(i, carry):
        p = 3 - i
        attend_rows(p)
        give_q(p).start()
        for copy in att_out(p):
            copy.start()

        @pl.when(i == 0)
        def _():
            w_copy.wait()
            w_first()
            give_q(3).wait_recv()
            lax.fori_loop(0, steps, pd_step, 0)
            for side in range(2):
                pd_write(side, steps - 1).wait()
                round1(side, steps - 1).start()
            w_first()
            arrive(1, X_NBR, 1)
            late(0).start()
            arrive(1, Y_NBR, 0)
            late(1).start()
            both(1, X_NBR ^ SIB)
            project_out(1)
            both(1, Y_NBR ^ SIB)
            project_out(2)

        return carry

    lax.fori_loop(0, 4, rows_step, 0)
    dkv[:, :BLK] = (dk_ref[...].T * scale).astype(BF16)
    dkv[:, BLK:] = dv_ref[...].T.astype(BF16)
    for p in range(3):
        give_q(p).wait_recv()
    for p in range(4):
        give_kv(p).start()

    def r_load(side, i):
        slot = lax.rem(2 * i + side, R_SLOTS)
        return pltpu.make_async_copy(r_ref.at[side, i], rt.at[slot], rt_sem.at[slot])

    def r_ahead(side, i):
        t = 2 * i + side + R_SLOTS - 1

        @pl.when(t < 2 * steps)
        def _():
            round1(lax.rem(t, 2), t // 2).wait_recv()
            r_load(lax.rem(t, 2), t // 2).start()

    groups = (1, 2, 0)
    targets = ((pxa_ref, pya_ref, poa_ref), (pxb_ref, pyb_ref, pob_ref))

    def p_writes(side, i):
        return [
            pltpu.make_async_copy(pt.at[side, pl.ds(g * BLK, BLK)], targets[side][g].at[i], pt_sem.at[side, g])
            for g in range(3)
        ]

    def p_step(i, carry):
        for side in range(2):
            w_load(side, i).wait()
            w_ahead(side, i)
            r_ahead(side, i)
            res = product(groups, side, i)

            @pl.when(i > 0)
            def _(side=side):
                for copy in p_writes(side, i - 1):
                    copy.wait()

            r_load(side, i).wait()
            add = 1 - side
            for g in range(3):
                rows = res[g * BLK : (g + 1) * BLK]
                pt[side, g * BLK : (g + 1) * BLK] = rows + rt[lax.rem(2 * i + side, R_SLOTS)] if g == add else rows
            for copy in p_writes(side, i):
                copy.start()

        return carry

    for t in range(R_SLOTS - 1):
        round1(t % 2, t // 2).wait_recv()
        r_load(t % 2, t // 2).start()
    for p in range(4):
        give_kv(p).wait_recv()
        kvs[p] = dkv[block_rows(p, core), :].astype(F32) + got_kv[p].astype(F32)
    p_step(0, 0)
    near = [
        remote(kvs.at[pl.ds(2 * i, 2)], dst, kn_send.at[n, i], kn_recv.at[n, i], mask)
        for n, (mask, dsts) in enumerate(((X_NBR, (kx0_ref, kx1_ref)), (Y_NBR, (ky0_ref, ky1_ref))))
        for i, dst in enumerate(dsts)
    ]
    for copy in near:
        copy.start()
    kv_out = pltpu.make_async_copy(kvs, kvo_ref, lsem.at[0])
    kv_out.start()
    lax.fori_loop(1, steps, p_step, 0)
    for side in range(2):
        for copy in p_writes(side, steps - 1):
            copy.wait()
    for copy in sends:
        copy.wait_send()
    for i in range(2):
        late(i).wait_send()
    for p in range(4):
        give_q(p).wait_send()
        give_kv(p).wait_send()
        for copy in att_out(p):
            copy.wait()
    for side in range(2):
        for i in range(steps):
            round1(side, i).wait_send()
    for copy in near:
        copy.wait()
    kv_out.wait()
    for t in range(2):
        for p in range(4):
            for copy in write_out(t, p):
                copy.wait()


TILE = 512
W_SLOTS = 4
R_SLOTS = 4


def front(x_blk, dy_blk, wq, wk, wv, wo, n_dev, scale):
    n_heads, dim, hd = wq.shape
    tokens = x_blk.shape[0] * n_dev
    wide = n_heads * hd
    steps = dim // 2 // TILE
    sds = jax.ShapeDtypeStruct
    sem = pltpu.SemaphoreType.DMA
    piece = sds((steps, BLK, TILE), F32)
    return pl.pallas_call(
        functools.partial(front_kernel, n_heads, scale),
        out_shape=(
            sds((tokens, dim), BF16), sds((tokens, dim), BF16), sds(wq.shape, BF16),
            sds((2, steps, BLK, TILE), F32), sds((2, steps, BLK, TILE), F32),
            piece, piece, piece, piece, piece, piece,
            sds((tokens, wide), BF16), sds((tokens, wide), BF16), sds((4, BLK, 2 * hd), F32),
        )
        + (sds((2, BLK, 2 * hd), F32),) * 4,
        in_specs=[ANY] * 6,
        out_specs=(ANY,) * 18,
        scratch_shapes=[
            pltpu.VMEM((n_dev, BLK, dim), BF16),
            pltpu.VMEM((n_dev, BLK, dim), BF16),
            pltpu.VMEM(wq.shape, BF16),
            pltpu.VMEM((max(2 * dim // TILE, W_SLOTS * n_heads), TILE, hd), BF16),
            pltpu.VMEM(wo.shape, BF16),
            pltpu.VMEM((tokens, wide), BF16),
            pltpu.VMEM((tokens, wide), BF16),
            pltpu.VMEM((tokens, wide), BF16),
            pltpu.VMEM((tokens, wide), BF16),
            pltpu.VMEM((tokens, hd), BF16),
            pltpu.VMEM((tokens, hd), BF16),
            pltpu.VMEM((hd, tokens), F32),
            pltpu.VMEM((hd, tokens), F32),
            pltpu.VMEM((2, 3 * BLK, TILE), F32),
            pltpu.VMEM((R_SLOTS, BLK, TILE), F32),
            pltpu.VMEM((4, BLK, wide), BF16),
            pltpu.VMEM((tokens, 2 * hd), BF16),
            pltpu.VMEM((4, BLK, 2 * hd), BF16),
            pltpu.VMEM((4, BLK, 2 * hd), F32),
            sem((2, 14)), sem((2, n_dev, 2)), sem((2,)), sem((6,)), sem((2, 4, 2)),
            sem((4,)), sem((4,)), sem((4,)), sem((4,)),
            sem((2, steps)), sem((2, steps)), sem((2, 2)), sem((2, 2)),
            sem((W_SLOTS,)), sem((2, 3)), sem((R_SLOTS,)), sem((4, 2)),
        ],
        compiler_params=pltpu.CompilerParams(collective_id=0, has_side_effects=True, vmem_limit_bytes=FULL),
        name="front",
    )(x_blk, dy_blk, wq, wk.reshape(-1, TILE, hd), wv.reshape(-1, TILE, hd), wo)


def dwo_kernel(o_ref, dy_ref, out_ref, o_t):
    @pl.when(pl.program_id(0) == 0)
    def _():
        o_t[...] = o_ref[...].T

    res = mm(o_t[...], dy_ref[...], 1, 0)
    for h in range(out_ref.shape[0]):
        out_ref[h] = res[h * BLK : (h + 1) * BLK]


def grad_wo(o, dy_full):
    tokens, wide = o.shape
    dim = dy_full.shape[1]
    tile = 512
    n_heads = wide // BLK
    return pl.pallas_call(
        dwo_kernel,
        grid=(dim // tile,),
        out_shape=jax.ShapeDtypeStruct((n_heads, BLK, dim), F32),
        in_specs=[pl.BlockSpec((tokens, wide), lambda j: (0, 0)), pl.BlockSpec((tokens, tile), lambda j: (0, j))],
        out_specs=pl.BlockSpec((n_heads, BLK, tile), lambda j: (0, 0, j)),
        scratch_shapes=[pltpu.VMEM((wide, tokens), BF16)],
        compiler_params=pltpu.CompilerParams(vmem_limit_bytes=FULL),
        cost_estimate=pl.CostEstimate(
            flops=2 * tokens * wide * dim, bytes_accessed=2 * tokens * dim + 4 * wide * dim, transcendentals=0
        ),
        name="grad_wo",
    )(o, dy_full)


def dwq_kernel(x_ref, dq_ref, out_ref):
    res = mm(x_ref[...], dq_ref[...], 0, 0)
    for h in range(out_ref.shape[0]):
        out_ref[h] = res[:, h * BLK : (h + 1) * BLK]


def grad_wq(x_full, dq):
    tokens, wide = dq.shape
    dim = x_full.shape[1]
    tile = 512
    n_heads = wide // BLK
    return pl.pallas_call(
        dwq_kernel,
        grid=(dim // tile,),
        out_shape=jax.ShapeDtypeStruct((n_heads, dim, BLK), F32),
        in_specs=[pl.BlockSpec((tokens, tile), lambda j: (0, j)), pl.BlockSpec((tokens, wide), lambda j: (0, 0))],
        out_specs=pl.BlockSpec((n_heads, tile, BLK), lambda j: (0, j, 0)),
        compiler_params=pltpu.CompilerParams(vmem_limit_bytes=FULL),
        cost_estimate=pl.CostEstimate(
            flops=2 * tokens * wide * dim, bytes_accessed=2 * tokens * dim + 4 * wide * dim, transcendentals=0
        ),
        name="grad_wq",
    )(x_full, dq)


def split3(a):
    hi = a.astype(BF16)
    rest = a - hi.astype(F32)
    mid = rest.astype(BF16)
    low = (rest - mid.astype(F32)).astype(BF16)
    return hi, mid, low


def kv_kernel(me_ref, mine_ref, other_ref, x_ref, dwk_ref, dwv_ref, rows_ref):
    me = me_ref[0]
    chip = me // 2
    core = lax.rem(me, 2)
    wide = mine_ref.shape[2]
    for p in range(4):
        chunk = jnp.bitwise_xor(chip, p)
        for ref, cls in ((mine_ref, core), (other_ref, 1 - core)):
            rows = pl.ds(pl.multiple_of(chunk * CHUNK + cls * BLK, BLK), BLK)
            for i, piece in enumerate(split3(ref[p])):
                rows_ref[rows, i * wide : (i + 1) * wide] = piece
    res = mm(x_ref[...], rows_ref[...], 0, 0)
    res = res[:, :wide] + res[:, wide : 2 * wide] + res[:, 2 * wide :]
    dwk_ref[...] = res[:, :BLK]
    dwv_ref[...] = res[:, BLK:]


def grad_kv(me, mine, other, x_full, n_dev):
    tokens, dim = x_full.shape
    own = dim // n_dev
    whole = pl.BlockSpec(mine.shape, lambda i, m: (0, 0, 0))
    out = pl.BlockSpec((own, BLK), lambda i, m: (0, 0))
    return pl.pallas_call(
        kv_kernel,
        grid_spec=pltpu.PrefetchScalarGridSpec(
            num_scalar_prefetch=1,
            grid=(1,),
            in_specs=[whole, whole, pl.BlockSpec((tokens, own), lambda i, m: (0, m[0]))],
            out_specs=(out, out),
            scratch_shapes=[pltpu.VMEM((tokens, 3 * mine.shape[2]), BF16)],
        ),
        out_shape=(jax.ShapeDtypeStruct((own, BLK), F32),) * 2,
        compiler_params=pltpu.CompilerParams(vmem_limit_bytes=FULL),
        cost_estimate=pl.CostEstimate(
            flops=2 * tokens * own * 3 * mine.shape[2], bytes_accessed=4 * tokens * own, transcendentals=0
        ),
        name="grad_kv",
    )(me, mine, other, x_full)


def kvdx_kernel(sum_ref, wka_ref, wkb_ref, wva_ref, wvb_ref, pa_ref, pb_ref, ra_ref, rb_ref, oa_ref, ob_ref):
    pieces = split3(sum_ref[0])
    for wk_ref, wv_ref, p_ref, r_ref, o_ref in (
        (wka_ref, wva_ref, pa_ref, ra_ref, oa_ref),
        (wkb_ref, wvb_ref, pb_ref, rb_ref, ob_ref),
    ):
        w = jnp.concatenate([wk_ref[...], wv_ref[...]], axis=1)
        res = mm(jnp.concatenate(pieces, axis=0), w, 1, 1)
        o_ref[...] = (p_ref[...] + r_ref[...]) + (res[:BLK] + res[BLK : 2 * BLK] + res[2 * BLK :])


def kv_dx(total, wk, wv, pa, pb, ra, rb):
    dim, hd = wk.shape
    steps, _, tile = pa.shape
    w_lo = pl.BlockSpec((tile, hd), lambda j: (j, 0))
    w_hi = pl.BlockSpec((tile, hd), lambda j: (j + steps, 0))
    col = pl.BlockSpec((None, BLK, tile), lambda j: (j, 0, 0))
    return pl.pallas_call(
        kvdx_kernel,
        grid=(steps,),
        out_shape=(jax.ShapeDtypeStruct(pa.shape, F32),) * 2,
        in_specs=[pl.BlockSpec((1,) + total.shape[1:], lambda j: (0, 0, 0)), w_lo, w_hi, w_lo, w_hi, col, col, col, col],
        out_specs=(col, col),
        compiler_params=pltpu.CompilerParams(vmem_limit_bytes=FULL),
        cost_estimate=pl.CostEstimate(flops=12 * BLK * dim * hd, bytes_accessed=10 * 2**20, transcendentals=0),
        name="kv_dx",
    )(total, wk, wk, wv, wv, pa, pb, ra, rb)


def dx_sum_kernel(a0, a1, b0, b1, out_ref, terms, res, in_sem, out_sem):
    steps, _, tile = a0.shape
    sides = ((a0, a1), (b0, b1))

    def load(side, i, n):
        return pltpu.make_async_copy(sides[side][n].at[i], terms.at[side, n, i], in_sem.at[side, n, i])

    def store(side, i):
        cols = pl.ds((side * steps + i) * tile, tile)
        return pltpu.make_async_copy(res.at[:, cols], out_ref.at[:, cols], out_sem.at[side, i])

    order = [(side, i) for side in range(2) for i in range(steps)]
    for side, i in order:
        for n in range(2):
            load(side, i, n).start()
    for side, i in order:
        for n in range(2):
            load(side, i, n).wait()
        at = (side * steps + i) * tile
        res[:, at : at + tile] = (terms[side, 0, i] + terms[side, 1, i]).astype(BF16)
        store(side, i).start()
    for side, i in order:
        store(side, i).wait()


def dx_sum(a_terms, b_terms):
    steps, rows, tile = a_terms[0].shape
    dim = 2 * steps * tile
    return pl.pallas_call(
        dx_sum_kernel,
        out_shape=jax.ShapeDtypeStruct((rows, dim), BF16),
        in_specs=[ANY] * 4,
        out_specs=ANY,
        scratch_shapes=[
            pltpu.VMEM((2, 2, steps, rows, tile), F32),
            pltpu.VMEM((rows, dim), BF16),
            pltpu.SemaphoreType.DMA((2, 2, steps)),
            pltpu.SemaphoreType.DMA((2, steps)),
        ],
        compiler_params=pltpu.CompilerParams(vmem_limit_bytes=FULL),
        cost_estimate=pl.CostEstimate(flops=2**20, bytes_accessed=8 * 2**20, transcendentals=0),
        name="dx_sum",
    )(*a_terms, *b_terms)


def solution(mesh):
    n_dev = mesh.shape["tp"]

    def swap(a, mask):
        return lax.ppermute(a, "tp", [(i, i ^ mask) for i in range(n_dev)])

    def local_grads(x_blk, dy_blk, wq_loc, w_k, w_v, wo_loc):
        n_heads, hd = wq_loc.shape[1:]
        scale = hd ** -0.5
        wide = n_heads * hd
        wq = jnp.transpose(wq_loc, (1, 0, 2))
        wk = w_k[:, 0, :]
        wv = w_v[:, 0, :]
        me = lax.axis_index("tp").astype(jnp.int32).reshape(1)
        (
            xf, dyf, _, _, _, px_a, px_b, py_a, py_b, po_a, po_b, o, dq, kvs, kx0, kx1, ky0, ky1
        ) = front(x_blk, dy_blk, wq, wk, wv, wo_loc, n_dev, scale)
        kd0 = swap(kx0, Y_NBR)
        kd1 = swap(ky1, X_NBR)
        a2 = swap(px_a, X_NBR)
        b2 = swap(py_b, Y_NBR)
        a3 = swap(py_a, Y_NBR)
        b3 = swap(px_b, X_NBR)
        dwo = grad_wo(o, dyf)
        kv_x = (kx0[0], kx0[1], kx1[0], kx1[1])
        kv_y = (ky0[0], ky0[1], ky1[0], ky1[1])
        kv_d = (kd0[0], kd0[1], kd1[0], kd1[1])
        total = jnp.stack([kvs[p] + kv_x[p ^ 1] + kv_y[p ^ 2] + kv_d[p ^ 3] for p in range(4)])
        other = swap(total, SIB)
        dwq = grad_wq(xf, dq)
        base_a, base_b = kv_dx(total, wk, wv, po_a, po_b, a2, b2)
        dwk, dwv = grad_kv(me, total, other, xf, n_dev)
        dx = dx_sum((base_a, a3), (base_b, b3))
        return dx, jnp.transpose(dwq, (1, 0, 2)), dwo, dwk, dwv

    tok_spec = P(("dp", "tp"))
    return jax.shard_map(
        local_grads,
        mesh=mesh,
        in_specs=(tok_spec, tok_spec, P(None, "tp", None), P(), P(), P("tp")),
        out_specs=(tok_spec, P("dp", "tp", None), tok_spec, tok_spec, tok_spec),
        check_vma=False,
    )
```
